128 devices in a mesh: fsdp: 32 (over x_hi, z, y), tensor: 4 (over x_lo, core).
Axes of the slice: x: 4 (x_hi: 2, x_lo: 2; x = x_hi * 2 + x_lo), y: 4, z: 4, core: 2. Of those that a mesh axis runs over, the one named last changes fastest.
Arguments:
- activations: bfloat16 [32768, 5120], P('fsdp', 'tensor'), may hold values from -6 to 6
- cotangent: bfloat16 [32768, 5120], P('fsdp', 'tensor'), may hold values from -0.032958984 to 0.032958984
- weights: float32 [5120, 5120], P(None, ('tensor', 'fsdp')), may hold values from -0.025 to 0.025
- first_moment: float32 [5120, 5120], P(None, ('tensor', 'fsdp')), may hold values from -3 to 3
- second_moment: float32 [5120, 5120], P(None, ('tensor', 'fsdp')), may hold values from 0.01 to 1
Outputs:
- weights_new: float32 [5120, 5120], P('fsdp', 'tensor')
- first_new: float32 [5120, 5120], P('fsdp', 'tensor')
- second_new: float32 [5120, 5120], P('fsdp', 'tensor')
- weights_bf16: bfloat16 [5120, 5120], P(None, 'tensor')
The draws below stay inside these ranges and needn't reach their ends.
All inputs are finite; a program needn't handle non-finite values.
Results may differ from the reference program's by a relative error of at most 0.014.
Values may be sent and summed in bfloat16 or wider, within the bound.
A program may use at most 128 MiB of HBM per device.

```python
import math
import jax
import jax.numpy as jnp
from jax import lax

D = 5120
TOK_DEV = 1024
STEP = 20
TOKENS = 32768
N_FSDP = 32


def with_spikes(array, key, source, target, parts, factor):
    owner, partner = [(jnp.arange(array.shape[dim]) // (array.shape[dim] // parts)).reshape([-1 if axis == dim else 1 for axis in range(array.ndim)]) for dim in (source, target)]
    chosen = jax.random.permutation(key, parts)[partner]
    strong = (owner == chosen) | (owner == (partner + parts // 2) % parts)
    return jnp.where(strong, factor * array, array)


def block_levels(key, extent, split, low, largest):
    factor_of = 1.0
    for dim, blocks in split:
        heights = jax.random.uniform(jax.random.fold_in(jax.random.fold_in(key, 6), dim), (blocks,), jnp.float32, low / len(split), largest / len(split))
        factor_of = factor_of * jnp.repeat(jnp.exp(heights), extent[dim] // blocks).reshape((-1,) + (1,) * (len(extent) - 1 - dim))
    return factor_of


def normal_values(stream_key, extent, scale, most, pieces=(), kind=jnp.bfloat16):
    array = scale * jax.random.normal(stream_key, extent, jnp.float32)
    if pieces:
        array = array * block_levels(stream_key, extent, pieces, -0.22, 0.18)
    return jnp.clip(array, -most, most).astype(kind)


def heavy_noise(own_key, dims, deviation, reach, split, heavy, dtype=jnp.bfloat16):
    values = deviation * jax.random.normal(own_key, dims, jnp.float32)
    if split:
        values = values * block_levels(own_key, dims, split, -0.22, 0.18)
    return jnp.clip(with_spikes(values, jax.random.fold_in(own_key, 3), *heavy), -reach, reach).astype(dtype)


def setup_inputs(seed: int = 0) -> dict:
    arg_keys = jax.random.split(jax.random.key(seed), 6)
    activations = heavy_noise(arg_keys[0], (TOKENS, D), 1.0, 6.0, ((0, 32), (1, 4)), (0, 1, 32, 2.75))
    cotangent = normal_values(arg_keys[1], (TOKENS, D), (1.0 / TOKENS ** 0.5), 0.032958984, ((0, 32), (1, 4)))
    weights = normal_values(arg_keys[2], (D, D), 0.004, 0.025, ((1, 128),), jnp.float32)
    first_moment = normal_values(arg_keys[3], (D, D), 0.5, 3.0, ((1, 128),), jnp.float32)
    second_moment = jnp.clip(jnp.exp(math.log(1.0) - 4.6051702 * jax.random.uniform(arg_keys[4], (D, D), jnp.float32) ** block_levels(arg_keys[4], (D, D), ((1, 128),), -0.2, 0.2)), 0.01, 1.0)
    return {"activations": activations, "cotangent": cotangent, "weights": weights, "first_moment": first_moment, "second_moment": second_moment}


beta_one = 0.9
beta_two = 0.95
adam_eps = 1e-08
learn_rate = 0.0003
decay_rate = 0.1

def adam_update(weights, first_moment, second_moment, gradient):
    first_new = beta_one * first_moment + (1.0 - beta_one) * gradient
    second_new = beta_two * second_moment + (1.0 - beta_two) * gradient * gradient
    corrected = first_new / (1.0 - beta_one ** STEP)
    scaled = jnp.sqrt(second_new / (1.0 - beta_two ** STEP)) + adam_eps
    weights_new = weights - learn_rate * (corrected / scaled + decay_rate * weights)
    return (weights_new, first_new, second_new)

def reference(activations, cotangent, weights, first_moment, second_moment):
    token_blocks = activations.reshape(N_FSDP, TOK_DEV, D)
    cotangent_blocks = cotangent.reshape(N_FSDP, TOK_DEV, D)

    def accumulate(running, block_pair):
        product = lax.dot_general(block_pair[0].astype(jnp.float32), block_pair[1].astype(jnp.float32), (((0,), (0,)), ((), ())))
        rounded = lax.optimization_barrier(product.astype(jnp.bfloat16))
        return (running + rounded.astype(jnp.float32), None)
    gradient, unused = lax.scan(accumulate, jnp.zeros((D, D), jnp.float32), (token_blocks, cotangent_blocks))
    weights_new, first_new, second_new = adam_update(weights, first_moment, second_moment, gradient)
    return (weights_new, first_new, second_new, weights_new.astype(jnp.bfloat16))
```

```python
import jax
import jax.numpy as jnp
from jax import lax
from jax.experimental import pallas as pl
from jax.experimental.pallas import tpu as pltpu
from jax.sharding import PartitionSpec as P

STEP = 20
D = 5120
BLOCK = 160
WAVES = 10
WIDE = 256
MESH = pl.DeviceIdType.MESH
BF = jnp.bfloat16

beta_one = 0.9
beta_two = 0.95
adam_eps = 1e-08
learn_rate = 0.0003
decay_rate = 0.1

ORDER = ((0, 2, 1, 3), (1, 3, 0, 2), (2, 1, 3, 0), (3, 0, 2, 1))
SLOT = (0, 8, 12, 14)


def adam_update(weights, first_moment, second_moment, gradient):
    first_new = beta_one * first_moment + (1.0 - beta_one) * gradient
    second_new = beta_two * second_moment + (1.0 - beta_two) * gradient * gradient
    corrected = first_new / (1.0 - beta_one**STEP)
    scaled = jnp.sqrt(second_new / (1.0 - beta_two**STEP)) + adam_eps
    weights_new = weights - learn_rate * (corrected / scaled + decay_rate * weights)
    return (weights_new, first_new, second_new)


def flip(value, dim):
    return value + 1 - 2 * (value % 2) if dim % 2 == 0 else 3 - value


def cube_bits(z, y):
    return ((y + y // 2) % 2, y // 2, (z + z // 2) % 2, z // 2)


def place(color, z, y):
    bits = cube_bits(z, y)
    order = ORDER[color]
    return bits[order[0]] * 8 + bits[order[1]] * 4 + bits[order[2]] * 2 + bits[order[3]]


def kernel(
    at_ref, c_ref, state_ref, wn_out, mn_out, vn_out, full_out,
    at, cot, part, recv, summed, final, full, state, fresh,
    load_sem, a_send, a_recv, c_send, c_recv, rs_send, rs_recv, x_send, x_recv, ag_send, ag_recv,
    gx_send, gx_recv, out_sem,
):
    f, t = lax.axis_index("fsdp"), lax.axis_index("tensor")
    hi, z, y = f // 16, (f // 4) % 4, f % 4
    lo, core = t // 2, t % 2

    def at_device(hi_, z_, y_, lo_, core_):
        return ((hi_ * 4 + z_) * 4 + y_, lo_ * 2 + core_)

    def cube_peer(dim):
        if dim < 2:
            return at_device(hi, z, flip(y, dim), lo, core)
        return at_device(hi, flip(z, dim), y, lo, core)

    def remote(src, dst, send, receive, device):
        return pltpu.make_async_remote_copy(
            src_ref=src, dst_ref=dst, send_sem=send, recv_sem=receive, device_id=device, device_id_type=MESH
        )

    bits = cube_bits(z, y)
    core_peer = at_device(hi, z, y, lo, 1 - core)
    lo_peer = at_device(hi, z, y, 1 - lo, core)
    hi_peer = at_device(1 - hi, z, y, lo, core)
    across = at_device(1 - hi, z, y, 1 - lo, core)

    barrier = pltpu.get_barrier_semaphore()
    greeted = [cube_peer(dim) for dim in range(4)] + [core_peer, lo_peer, hi_peer, across]
    for device in greeted:
        pl.semaphore_signal(barrier, inc=1, device_id=device, device_id_type=MESH)
    pl.semaphore_wait(barrier, len(greeted))

    mine = pl.ds(pl.multiple_of(core * 1280, 128), 1280)
    send_a = remote(at_ref, at.at[mine], a_send, a_recv, core_peer)
    send_a.start()
    load_a = pltpu.make_async_copy(at_ref, at.at[mine], load_sem.at[0])
    load_a.start()
    load_c = [
        pltpu.make_async_copy(c_ref.at[:, pl.ds(WIDE * k, WIDE)], cot.at[k], load_sem.at[1 + k]) for k in range(5)
    ]
    for k in range(5):
        load_c[k].start()
    send_c = [
        remote(c_ref.at[:, pl.ds(WIDE * k, WIDE)], cot.at[5 + k], c_send.at[k], c_recv.at[k], lo_peer)
        for k in range(5)
    ]
    for k in range(5):
        send_c[k].start()
    load_s = pltpu.make_async_copy(state_ref, state, load_sem.at[6])
    load_s.start()
    load_a.wait()
    for k in range(5):
        load_c[k].wait()
    load_s.wait()
    send_a.wait_recv()

    def base(color, stage):
        total = 0
        for s in range(stage):
            total = total + bits[ORDER[color][s]] * (8 >> s)
        return total

    def halving(wave, color, stage):
        half = 8 >> stage
        dim = ORDER[color][stage]
        return remote(
            part.at[wave, color, pl.ds(base(color, stage) + (1 - bits[dim]) * half, half)],
            recv.at[wave, color, pl.ds(SLOT[stage], half)],
            rs_send,
            rs_recv.at[wave, stage, color],
            cube_peer(dim),
        )

    def add(wave, color, stage, which):
        half = 8 >> stage
        bit = bits[ORDER[color][stage]]
        shift = (1 - bit if which else bit) * half
        own = pl.ds(base(color, stage) + shift, half)
        came = pl.ds(SLOT[stage - 1] + shift, half)
        part[wave, color, own] = (
            part[wave, color, own].astype(jnp.float32) + recv[wave, color, came].astype(jnp.float32)
        ).astype(BF)

    def x_target(wave):
        column = jnp.where(wave < 5, lo, 1 - lo)
        return at_device(lo, z, y, column, core)

    def x_copy(wave):
        k = wave % 5
        return remote(summed.at[wave], final.at[hi, k], x_send.at[wave], x_recv.at[hi, k], x_target(wave))

    stays = hi == lo

    def tick(now, carry):
        wave_4 = now - 5

        @pl.when((wave_4 >= 0) & (wave_4 < WAVES))
        def _():
            for color in range(4):
                halving(wave_4, color, 3).wait_recv()
                summed[wave_4, color] = (
                    part[wave_4, color, base(color, 4)].astype(jnp.float32)
                    + recv[wave_4, color, SLOT[3]].astype(jnp.float32)
                ).astype(BF)

            @pl.when(stays & (wave_4 < 5))
            def _():
                final[hi, wave_4 % 5] = summed[wave_4]

            @pl.when(jnp.logical_not(stays & (wave_4 < 5)))
            def _():
                x_copy(wave_4).start()

        for stage in (3, 2, 1):
            wave = now - 1 - stage

            @pl.when((wave >= 0) & (wave < WAVES))
            def _(wave=wave, stage=stage):
                for color in range(4):
                    halving(wave, color, stage - 1).wait_recv()
                    add(wave, color, stage, 1)
                    halving(wave, color, stage).start()
                    add(wave, color, stage, 0)

        @pl.when(now < WAVES)
        def _():
            for k in range(5):
                @pl.when(now == 5 + k)
                def _(k=k):
                    send_c[k].wait_recv()

            def rows(quarter, carry):
                left = at[pl.ds(pl.multiple_of(quarter * 640, 128), 640), :]
                product = jnp.dot(left, cot[now], preferred_element_type=jnp.float32).astype(BF)
                for i in range(4):
                    for color in range(4):
                        top, side = i * BLOCK + (color // 2) * 80, (color % 2) * 128
                        part[now, color, place(color, quarter, i)] = product[top : top + 80, side : side + 128]
                return carry

            lax.fori_loop(0, 4, rows, 0)
            for color in range(4):
                halving(now, color, 0).start()

        return carry

    lax.fori_loop(0, WAVES + 5, tick, 0)

    my_rows = pl.multiple_of(f * BLOCK, BLOCK)

    def update(k, carry):
        for source in range(2):
            @pl.when(jnp.logical_not(stays & (hi == source)))
            def _(source=source):
                pltpu.make_async_copy(final.at[source, k], final.at[source, k], x_recv.at[source, k]).wait()

        for color in range(4):
            rows = pl.ds((color // 2) * 80, 80)
            columns = pl.ds(pl.multiple_of(k * WIDE + (color % 2) * 128, 128), 128)
            gradient = final[0, k, color].astype(jnp.float32) + final[1, k, color].astype(jnp.float32)
            new = adam_update(*(state[i, rows, columns].astype(jnp.float32) for i in range(3)), gradient)
            for i in range(3):
                fresh[i, rows, columns] = new[i]
            full[pl.ds(my_rows + (color // 2) * 80, 80), columns] = new[0].astype(BF)
        return carry

    lax.fori_loop(0, 5, update, 0)

    def block(x, color, number):
        z_, y_ = z, y
        order = ORDER[color][::-1]
        for i in range(4):
            if number >> i & 1:
                dim = order[i]
                if dim < 2:
                    y_ = flip(y_, dim)
                else:
                    z_ = flip(z_, dim)
        owner = ((1 - hi if x else hi) * 4 + z_) * 4 + y_
        rows = pl.ds(pl.multiple_of(owner * BLOCK + (color // 2) * 80, 16), 80)
        return full.at[rows, pl.ds((color % 2) * 640, 640)]

    def forward(x, color, number, i):
        here = block(x, color, number)
        return remote(
            here, here, ag_send, ag_recv.at[x, color, number + (1 << i)], cube_peer(ORDER[color][::-1][i])
        )

    def arrived(x, color, number):
        here = block(x, color, number)
        pltpu.make_async_copy(here, here, ag_recv.at[x, color, number]).wait()

    own_rows = full.at[pl.ds(my_rows, BLOCK)]
    to_hi = remote(own_rows, own_rows, gx_send, gx_recv, hi_peer)
    to_hi.start()
    for color in range(4):
        for i in (3, 2, 1, 0):
            forward(0, color, 0, i).start()
    stores = [
        pltpu.make_async_copy(fresh.at[i], out, out_sem.at[i]) for i, out in enumerate((wn_out, mn_out, vn_out))
    ]
    for store in stores:
        store.start()
    for number in range(1, 8):
        for color in range(4):
            arrived(0, color, number)
            for i in (3, 2, 1):
                if number < 1 << i:
                    forward(0, color, number, i).start()
    to_hi.wait_recv()
    for color in range(4):
        for i in (3, 2, 1, 0):
            forward(1, color, 0, i).start()
    for number in range(8, 16):
        for color in range(4):
            arrived(0, color, number)
    near = pl.ds(pl.multiple_of(hi * 2560, 128), 2560)
    far = pl.ds(pl.multiple_of((1 - hi) * 2560, 128), 2560)
    store_near = pltpu.make_async_copy(full.at[near], full_out.at[near], out_sem.at[3])
    store_near.start()
    for number in range(1, 8):
        for color in range(4):
            arrived(1, color, number)
            for i in (3, 2, 1):
                if number < 1 << i:
                    forward(1, color, number, i).start()
    for number in range(8, 16):
        for color in range(4):
            arrived(1, color, number)
    store_far = pltpu.make_async_copy(full.at[far], full_out.at[far], out_sem.at[4])
    store_far.start()

    send_a.wait_send()
    for k in range(5):
        send_c[k].wait_send()
    pltpu.make_async_copy(recv, recv, rs_send).wait()
    for wave in range(WAVES):
        if wave < 5:
            @pl.when(jnp.logical_not(stays))
            def _(wave=wave):
                x_copy(wave).wait_send()
        else:
            x_copy(wave).wait_send()
    to_hi.wait_send()
    pltpu.make_async_copy(full.at[pl.ds(0, 4800)], full.at[pl.ds(0, 4800)], ag_send).wait()
    for store in stores:
        store.wait()
    store_near.wait()
    store_far.wait()


def body(activations, cotangent, weights, first_moment, second_moment):
    packed = jnp.concatenate([weights, first_moment, second_moment], axis=1).astype(BF)
    moved = lax.all_to_all(packed.reshape(32, BLOCK, 120), "fsdp", 0, 0, tiled=True)
    state = moved.reshape(32, BLOCK, 3, 40).transpose(2, 1, 0, 3).reshape(3, BLOCK, 1280)
    any_space = pl.BlockSpec(memory_space=pl.ANY)
    shard = jax.ShapeDtypeStruct((BLOCK, 1280), jnp.float32)
    dma = pltpu.SemaphoreType.DMA
    return pl.pallas_call(
        kernel,
        name="step",
        out_shape=(shard, shard, shard, jax.ShapeDtypeStruct((D, 1280), BF)),
        in_specs=[any_space] * 3,
        out_specs=(any_space,) * 4,
        scratch_shapes=[
            pltpu.VMEM((2560, 1024), BF),
            pltpu.VMEM((10, 1024, WIDE), BF),
            pltpu.VMEM((WAVES, 4, 16, 80, 128), BF),
            pltpu.VMEM((WAVES, 4, 15, 80, 128), BF),
            pltpu.VMEM((WAVES, 4, 80, 128), BF),
            pltpu.VMEM((2, 5, 4, 80, 128), BF),
            pltpu.VMEM((D, 1280), BF),
            pltpu.VMEM((3, BLOCK, 1280), BF),
            pltpu.VMEM((3, BLOCK, 1280), jnp.float32),
            dma((7,)), dma, dma, dma((5,)), dma((5,)), dma, dma((WAVES, 4, 4)), dma((WAVES,)), dma((2, 5)),
            dma, dma((2, 4, 16)), dma, dma, dma((5,)),
        ],
        compiler_params=pltpu.CompilerParams(
            collective_id=0, has_side_effects=True, vmem_limit_bytes=67043328
        ),
        cost_estimate=pl.CostEstimate(flops=13_421_772_800, bytes_accessed=40_000_000, transcendentals=0),
    )(activations.T, cotangent, state)


def solution(mesh):
    return jax.shard_map(
        body,
        mesh=mesh,
        in_specs=(
            P("fsdp", "tensor"),
            P("fsdp", "tensor"),
            P(None, ("tensor", "fsdp")),
            P(None, ("tensor", "fsdp")),
            P(None, ("tensor", "fsdp")),
        ),
        out_specs=(
            P("fsdp", "tensor"),
            P("fsdp", "tensor"),
            P("fsdp", "tensor"),
            P(None, "tensor"),
        ),
        check_vma=False,
    )
```

```python
import jax
import jax.numpy as jnp
from jax import lax
from jax.experimental import pallas as pl
from jax.experimental.pallas import tpu as pltpu
from jax.sharding import PartitionSpec as P

STEP = 20
D = 5120
BLOCK = 160
WAVES = 10
WIDE = 256
MESH = pl.DeviceIdType.MESH
BF = jnp.bfloat16

beta_one = 0.9
beta_two = 0.95
adam_eps = 1e-08
learn_rate = 0.0003
decay_rate = 0.1

ORDER = ((0, 2, 1, 3), (1, 3, 0, 2), (2, 1, 3, 0), (3, 0, 2, 1))
SLOT = (0, 8, 12, 14)


def adam_update(weights, first_moment, second_moment, gradient):
    first_new = beta_one * first_moment + (1.0 - beta_one) * gradient
    second_new = beta_two * second_moment + (1.0 - beta_two) * gradient * gradient
    corrected = first_new / (1.0 - beta_one**STEP)
    scaled = jnp.sqrt(second_new / (1.0 - beta_two**STEP)) + adam_eps
    weights_new = weights - learn_rate * (corrected / scaled + decay_rate * weights)
    return (weights_new, first_new, second_new)


def flip(value, dim):
    return value + 1 - 2 * (value % 2) if dim % 2 == 0 else 3 - value


def cube_bits(z, y):
    return ((y + y // 2) % 2, y // 2, (z + z // 2) % 2, z // 2)


def place(color, z, y):
    bits = cube_bits(z, y)
    order = ORDER[color]
    return bits[order[0]] * 8 + bits[order[1]] * 4 + bits[order[2]] * 2 + bits[order[3]]


def kernel(
    a_ref, c_ref, w_ref, m_ref, v_ref, wn_out, mn_out, vn_out, full_out,
    at, cot, part, recv, summed, final, full, fresh, tall, packed, moved,
    load_sem, s_send, s_recv, a_send, a_recv, c_send, c_recv, rs_send, rs_recv, x_send, x_recv, ag_send, ag_recv,
    gx_send, gx_recv, out_sem,
):
    f, t = lax.axis_index("fsdp"), lax.axis_index("tensor")
    hi, z, y = f // 16, (f // 4) % 4, f % 4
    lo, core = t // 2, t % 2

    def at_device(hi_, z_, y_, lo_, core_):
        return ((hi_ * 4 + z_) * 4 + y_, lo_ * 2 + core_)

    def cube_peer(dim):
        if dim < 2:
            return at_device(hi, z, flip(y, dim), lo, core)
        return at_device(hi, flip(z, dim), y, lo, core)

    def remote(src, dst, send, receive, device):
        return pltpu.make_async_remote_copy(
            src_ref=src, dst_ref=dst, send_sem=send, recv_sem=receive, device_id=device, device_id_type=MESH
        )

    bits = cube_bits(z, y)
    core_peer = at_device(hi, z, y, lo, 1 - core)
    lo_peer = at_device(hi, z, y, 1 - lo, core)
    hi_peer = at_device(1 - hi, z, y, lo, core)
    across = at_device(1 - hi, z, y, 1 - lo, core)

    barrier = pltpu.get_barrier_semaphore()
    for device in (core_peer, lo_peer, across):
        pl.semaphore_signal(barrier, inc=1, device_id=device, device_id_type=MESH)

    def greet(step, carry):
        pl.semaphore_signal(barrier, inc=1, device_id=((f + step) % 32, t), device_id_type=MESH)
        return carry

    lax.fori_loop(1, 32, greet, 0)
    pl.semaphore_wait(barrier, 34)

    near_row = pl.multiple_of(hi * 2560, 128)
    raw = [full.at[pl.ds(near_row, 1024)], full.at[pl.ds(near_row + 1024, 1024)]]
    send_a = remote(a_ref, raw[1], a_send, a_recv, core_peer)
    load_a = pltpu.make_async_copy(a_ref, raw[0], load_sem.at[0])
    load_a.start()
    send_a.start()
    load_s = [
        pltpu.make_async_copy(ref, tall.at[pl.ds(40 * i, 40)], load_sem.at[6 + i])
        for i, ref in enumerate((w_ref, m_ref, v_ref))
    ]
    for load in load_s:
        load.start()
    load_c = [
        pltpu.make_async_copy(c_ref.at[:, pl.ds(WIDE * k, WIDE)], cot.at[k], load_sem.at[1 + k]) for k in range(5)
    ]
    for k in range(5):
        load_c[k].start()
    send_c = [
        remote(c_ref.at[:, pl.ds(WIDE * k, WIDE)], cot.at[5 + k], c_send.at[k], c_recv.at[k], lo_peer)
        for k in range(5)
    ]
    for k in range(5):
        send_c[k].start()

    def turn(start, core_):
        def step(i, carry):
            columns = pl.ds(pl.multiple_of(i * 128, 128), 128)
            rows = pl.ds(pl.multiple_of(core_ * 1280 + i * 128, 128), 128)
            at[rows, :] = full[pl.ds(start, 1024), columns].T
            return carry

        lax.fori_loop(0, 10, step, 0)

    load_a.wait()
    turn(near_row, core)

    tall[pl.ds(120, 8), :] = jnp.zeros((8, D), jnp.float32)
    for load in load_s:
        load.wait()

    def pack(i, carry):
        packed[pl.ds(pl.multiple_of(i * 512, 512), 512), :] = tall[:, pl.ds(pl.multiple_of(i * 512, 512), 512)].T.astype(BF)
        return carry

    lax.fori_loop(0, 10, pack, 0)

    def own_state(owner):
        return packed.at[pl.ds(pl.multiple_of(owner * BLOCK, BLOCK), BLOCK)]

    def send_state(step, carry):
        owner = (f + step) % 32
        remote(own_state(owner), moved.at[f], s_send, s_recv, (owner, t)).start()
        return carry

    lax.fori_loop(1, 32, send_state, 0)
    moved[f] = packed[pl.ds(pl.multiple_of(f * BLOCK, BLOCK), BLOCK), :]
    for k in range(5):
        load_c[k].wait()

    def spread():
        pltpu.make_async_copy(moved.at[pl.ds(0, 31)], moved.at[pl.ds(0, 31)], s_recv).wait()
        lane = lax.broadcasted_iota(jnp.int32, (BLOCK, 128), 1)

        def half(h, carry):
            for group in range(5):
                value = [jnp.zeros((BLOCK, 128), jnp.float32)] * 3
                for g in range(16):
                    left = 40 * g - 128 * group
                    if left <= -40 or left >= 128:
                        continue
                    piece = moved[h * 16 + g].astype(jnp.float32)
                    here = (lane >= left) & (lane < left + 40)
                    for i in range(3):
                        shift = (left - 40 * i) % 128
                        rolled = pltpu.roll(piece, shift, 1) if shift else piece
                        value[i] = jnp.where(here, rolled, value[i])
                for i in range(3):
                    fresh[i, :, pl.ds(pl.multiple_of(h * 640 + group * 128, 128), 128)] = value[i]
            return carry

        lax.fori_loop(0, 2, half, 0)

    def base(color, stage):
        total = 0
        for s in range(stage):
            total = total + bits[ORDER[color][s]] * (8 >> s)
        return total

    def halving(wave, color, stage):
        half = 8 >> stage
        dim = ORDER[color][stage]
        return remote(
            part.at[wave, color, pl.ds(base(color, stage) + (1 - bits[dim]) * half, half)],
            recv.at[wave, color, pl.ds(SLOT[stage], half)],
            rs_send,
            rs_recv.at[wave, stage, color],
            cube_peer(dim),
        )

    def add(wave, color, stage, which):
        half = 8 >> stage
        bit = bits[ORDER[color][stage]]
        shift = (1 - bit if which else bit) * half
        own = pl.ds(base(color, stage) + shift, half)
        came = pl.ds(SLOT[stage - 1] + shift, half)
        part[wave, color, own] = (
            part[wave, color, own].astype(jnp.float32) + recv[wave, color, came].astype(jnp.float32)
        ).astype(BF)

    def x_target(wave):
        column = jnp.where(wave < 5, lo, 1 - lo)
        return at_device(lo, z, y, column, core)

    def x_copy(wave):
        k = wave % 5
        return remote(summed.at[wave], final.at[hi, k], x_send.at[wave], x_recv.at[hi, k], x_target(wave))

    stays = hi == lo

    def tick(now, carry):
        wave_4 = now - 5

        @pl.when((wave_4 >= 0) & (wave_4 < WAVES))
        def _():
            for color in range(4):
                halving(wave_4, color, 3).wait_recv()
                summed[wave_4, color] = (
                    part[wave_4, color, base(color, 4)].astype(jnp.float32)
                    + recv[wave_4, color, SLOT[3]].astype(jnp.float32)
                ).astype(BF)

            @pl.when(stays & (wave_4 < 5))
            def _():
                final[hi, wave_4 % 5] = summed[wave_4]

            @pl.when(jnp.logical_not(stays & (wave_4 < 5)))
            def _():
                x_copy(wave_4).start()

        for stage in (3, 2, 1):
            wave = now - 1 - stage

            @pl.when((wave >= 0) & (wave < WAVES))
            def _(wave=wave, stage=stage):
                for color in range(4):
                    halving(wave, color, stage - 1).wait_recv()
                    add(wave, color, stage, 1)
                    halving(wave, color, stage).start()
                    add(wave, color, stage, 0)

        @pl.when(now < WAVES)
        def _():
            for k in range(5):
                @pl.when(now == 5 + k)
                def _(k=k):
                    send_c[k].wait_recv()

            def rows(step, carry):
                @pl.when((now == 0) & (step == 2))
                def _():
                    send_a.wait_recv()
                    turn(near_row + 1024, 1 - core)

                quarter = (core * 2 + step) % 4
                left = at[pl.ds(pl.multiple_of(quarter * 640, 128), 640), :]
                product = jnp.dot(left, cot[now], preferred_element_type=jnp.float32).astype(BF)
                for i in range(4):
                    for color in range(4):
                        top, side = i * BLOCK + (color // 2) * 80, (color % 2) * 128
                        part[now, color, place(color, quarter, i)] = product[top : top + 80, side : side + 128]
                return carry

            lax.fori_loop(0, 4, rows, 0)
            for color in range(4):
                halving(now, color, 0).start()

        @pl.when(now == 7)
        def _():
            spread()

        return carry

    lax.fori_loop(0, WAVES + 5, tick, 0)

    my_rows = pl.multiple_of(f * BLOCK, BLOCK)

    def update(k, carry):
        for source in range(2):
            @pl.when(jnp.logical_not(stays & (hi == source)))
            def _(source=source):
                pltpu.make_async_copy(final.at[source, k], final.at[source, k], x_recv.at[source, k]).wait()

        for color in range(4):
            rows = pl.ds((color // 2) * 80, 80)
            columns = pl.ds(pl.multiple_of(k * WIDE + (color % 2) * 128, 128), 128)
            gradient = final[0, k, color].astype(jnp.float32) + final[1, k, color].astype(jnp.float32)
            new = adam_update(*(fresh[i, rows, columns] for i in range(3)), gradient)
            for i in range(3):
                fresh[i, rows, columns] = new[i]
            full[pl.ds(my_rows + (color // 2) * 80, 80), columns] = new[0].astype(BF)
        return carry

    lax.fori_loop(0, 5, update, 0)

    def block(x, color, number):
        z_, y_ = z, y
        order = ORDER[color][::-1]
        for i in range(4):
            if number >> i & 1:
                dim = order[i]
                if dim < 2:
                    y_ = flip(y_, dim)
                else:
                    z_ = flip(z_, dim)
        owner = ((1 - hi if x else hi) * 4 + z_) * 4 + y_
        rows = pl.ds(pl.multiple_of(owner * BLOCK + (color // 2) * 80, 16), 80)
        return full.at[rows, pl.ds((color % 2) * 640, 640)]

    def forward(x, color, number, i):
        here = block(x, color, number)
        return remote(
            here, here, ag_send, ag_recv.at[x, color, number + (1 << i)], cube_peer(ORDER[color][::-1][i])
        )

    def arrived(x, color, number):
        here = block(x, color, number)
        pltpu.make_async_copy(here, here, ag_recv.at[x, color, number]).wait()

    own_rows = full.at[pl.ds(my_rows, BLOCK)]
    to_hi = remote(own_rows, own_rows, gx_send, gx_recv, hi_peer)
    to_hi.start()
    for color in range(4):
        for i in (3, 2, 1, 0):
            forward(0, color, 0, i).start()
    stores = [
        pltpu.make_async_copy(fresh.at[i], out, out_sem.at[i]) for i, out in enumerate((wn_out, mn_out, vn_out))
    ]
    for store in stores:
        store.start()
    for number in range(1, 8):
        for color in range(4):
            arrived(0, color, number)
            for i in (3, 2, 1):
                if number < 1 << i:
                    forward(0, color, number, i).start()
    to_hi.wait_recv()
    for color in range(4):
        for i in (3, 2, 1, 0):
            forward(1, color, 0, i).start()
    for number in range(8, 16):
        for color in range(4):
            arrived(0, color, number)
    near = pl.ds(pl.multiple_of(hi * 2560, 128), 2560)
    far = pl.ds(pl.multiple_of((1 - hi) * 2560, 128), 2560)
    store_near = pltpu.make_async_copy(full.at[near], full_out.at[near], out_sem.at[3])
    store_near.start()
    for number in range(1, 8):
        for color in range(4):
            arrived(1, color, number)
            for i in (3, 2, 1):
                if number < 1 << i:
                    forward(1, color, number, i).start()
    for number in range(8, 16):
        for color in range(4):
            arrived(1, color, number)
    store_far = pltpu.make_async_copy(full.at[far], full_out.at[far], out_sem.at[4])
    store_far.start()

    send_a.wait_send()
    pltpu.make_async_copy(packed.at[pl.ds(0, 4960)], packed.at[pl.ds(0, 4960)], s_send).wait()
    for k in range(5):
        send_c[k].wait_send()
    pltpu.make_async_copy(recv, recv, rs_send).wait()
    for wave in range(WAVES):
        if wave < 5:
            @pl.when(jnp.logical_not(stays))
            def _(wave=wave):
                x_copy(wave).wait_send()
        else:
            x_copy(wave).wait_send()
    to_hi.wait_send()
    pltpu.make_async_copy(full.at[pl.ds(0, 4800)], full.at[pl.ds(0, 4800)], ag_send).wait()
    for store in stores:
        store.wait()
    store_near.wait()
    store_far.wait()


def body(activations, cotangent, weights, first_moment, second_moment):
    any_space = pl.BlockSpec(memory_space=pl.ANY)
    shard = jax.ShapeDtypeStruct((BLOCK, 1280), jnp.float32)
    dma = pltpu.SemaphoreType.DMA
    return pl.pallas_call(
        kernel,
        name="step",
        out_shape=(shard, shard, shard, jax.ShapeDtypeStruct((D, 1280), BF)),
        in_specs=[any_space] * 5,
        out_specs=(any_space,) * 4,
        scratch_shapes=[
            pltpu.VMEM((2560, 1024), BF),
            pltpu.VMEM((10, 1024, WIDE), BF),
            pltpu.VMEM((WAVES, 4, 16, 80, 128), BF),
            pltpu.VMEM((WAVES, 4, 15, 80, 128), BF),
            pltpu.VMEM((WAVES, 4, 80, 128), BF),
            pltpu.VMEM((2, 5, 4, 80, 128), BF),
            pltpu.VMEM((D, 1280), BF),
            pltpu.VMEM((3, BLOCK, 1280), jnp.float32),
            pltpu.VMEM((128, D), jnp.float32),
            pltpu.VMEM((D, 128), BF),
            pltpu.VMEM((32, BLOCK, 128), BF),
            dma((9,)), dma, dma, dma, dma, dma((5,)), dma((5,)), dma, dma((WAVES, 4, 4)), dma((WAVES,)), dma((2, 5)),
            dma, dma((2, 4, 16)), dma, dma, dma((5,)),
        ],
        compiler_params=pltpu.CompilerParams(
            collective_id=0, has_side_effects=True, vmem_limit_bytes=67043328
        ),
        cost_estimate=pl.CostEstimate(flops=13_421_772_800, bytes_accessed=40_000_000, transcendentals=0),
    )(activations, cotangent, weights.T, first_moment.T, second_moment.T)


def solution(mesh):
    return jax.shard_map(
        body,
        mesh=mesh,
        in_specs=(
            P("fsdp", "tensor"),
            P("fsdp", "tensor"),
            P(None, ("tensor", "fsdp")),
            P(None, ("tensor", "fsdp")),
            P(None, ("tensor", "fsdp")),
        ),
        out_specs=(
            P("fsdp", "tensor"),
            P("fsdp", "tensor"),
            P("fsdp", "tensor"),
            P(None, "tensor"),
        ),
        check_vma=False,
    )
```

```python
import jax
import jax.numpy as jnp
from jax import lax
from jax.experimental import pallas as pl
from jax.experimental.pallas import tpu as pltpu
from jax.sharding import PartitionSpec as P

STEP = 20
D = 5120
BLOCK = 160
WAVES = 10
WIDE = 256
MESH = pl.DeviceIdType.MESH
BF = jnp.bfloat16

beta_one = 0.9
beta_two = 0.95
adam_eps = 1e-08
learn_rate = 0.0003
decay_rate = 0.1

ORDER = ((0, 2, 1, 3), (1, 3, 0, 2), (2, 1, 3, 0), (3, 0, 2, 1))
SLOT = (0, 8, 12, 14)


def adam_update(weights, first_moment, second_moment, gradient):
    first_new = beta_one * first_moment + (1.0 - beta_one) * gradient
    second_new = beta_two * second_moment + (1.0 - beta_two) * gradient * gradient
    corrected = first_new / (1.0 - beta_one**STEP)
    scaled = jnp.sqrt(second_new / (1.0 - beta_two**STEP)) + adam_eps
    weights_new = weights - learn_rate * (corrected / scaled + decay_rate * weights)
    return (weights_new, first_new, second_new)


def flip(value, dim):
    return value + 1 - 2 * (value % 2) if dim % 2 == 0 else 3 - value


def cube_bits(z, y):
    return ((y + y // 2) % 2, y // 2, (z + z // 2) % 2, z // 2)


def place(color, z, y):
    bits = cube_bits(z, y)
    order = ORDER[color]
    return bits[order[0]] * 8 + bits[order[1]] * 4 + bits[order[2]] * 2 + bits[order[3]]


def kernel(
    a_ref, c_ref, w_ref, m_ref, v_ref, wn_out, mn_out, vn_out, full_out,
    at, cot, part, recv, summed, final, full, fresh, tall, packed, moved,
    load_sem, s_send, s_recv, a_send, a_recv, c_send, c_recv, rs_send, rs_recv, x_send, x_recv, ag_send, ag_recv,
    gx_send, out_sem,
):
    f, t = lax.axis_index("fsdp"), lax.axis_index("tensor")
    hi, z, y = f // 16, (f // 4) % 4, f % 4
    lo, core = t // 2, t % 2

    def at_device(hi_, z_, y_, lo_, core_):
        return ((hi_ * 4 + z_) * 4 + y_, lo_ * 2 + core_)

    def cube_peer(dim):
        if dim < 2:
            return at_device(hi, z, flip(y, dim), lo, core)
        return at_device(hi, flip(z, dim), y, lo, core)

    def remote(src, dst, send, receive, device):
        return pltpu.make_async_remote_copy(
            src_ref=src, dst_ref=dst, send_sem=send, recv_sem=receive, device_id=device, device_id_type=MESH
        )

    bits = cube_bits(z, y)
    core_peer = at_device(hi, z, y, lo, 1 - core)
    lo_peer = at_device(hi, z, y, 1 - lo, core)
    hi_peer = at_device(1 - hi, z, y, lo, core)
    across = at_device(1 - hi, z, y, 1 - lo, core)

    barrier = pltpu.get_barrier_semaphore()
    for device in (core_peer, lo_peer, across):
        pl.semaphore_signal(barrier, inc=1, device_id=device, device_id_type=MESH)

    def greet(step, carry):
        pl.semaphore_signal(barrier, inc=1, device_id=((f + step) % 32, t), device_id_type=MESH)
        return carry

    lax.fori_loop(1, 32, greet, 0)
    pl.semaphore_wait(barrier, 34)

    near_row = pl.multiple_of(hi * 2560, 128)
    raw = [full.at[pl.ds(near_row, 1024)], full.at[pl.ds(near_row + 1024, 1024)]]
    send_a = remote(a_ref, raw[1], a_send, a_recv, core_peer)
    load_a = pltpu.make_async_copy(a_ref, raw[0], load_sem.at[0])
    load_a.start()
    send_a.start()
    load_s = [
        pltpu.make_async_copy(ref, tall.at[pl.ds(40 * i, 40)], load_sem.at[6 + i])
        for i, ref in enumerate((w_ref, m_ref, v_ref))
    ]
    for load in load_s:
        load.start()
    load_c = [
        pltpu.make_async_copy(c_ref.at[:, pl.ds(WIDE * k, WIDE)], cot.at[k], load_sem.at[1 + k]) for k in range(5)
    ]
    for k in range(5):
        load_c[k].start()
    send_c = [
        remote(c_ref.at[:, pl.ds(WIDE * k, WIDE)], cot.at[5 + k], c_send.at[k], c_recv.at[k], lo_peer)
        for k in range(5)
    ]
    send_c[0].start()
    send_c[1].start()

    def turn(start, core_):
        def step(i, carry):
            columns = pl.ds(pl.multiple_of(i * 128, 128), 128)
            rows = pl.ds(pl.multiple_of(core_ * 1280 + i * 128, 128), 128)
            at[rows, :] = full[pl.ds(start, 1024), columns].T
            return carry

        lax.fori_loop(0, 10, step, 0)

    load_a.wait()
    turn(near_row, core)

    tall[pl.ds(120, 8), :] = jnp.zeros((8, D), jnp.float32)
    for load in load_s:
        load.wait()

    def pack(i, carry):
        packed[pl.ds(pl.multiple_of(i * 512, 512), 512), :] = tall[:, pl.ds(pl.multiple_of(i * 512, 512), 512)].T.astype(BF)
        return carry

    lax.fori_loop(0, 10, pack, 0)

    def own_state(owner):
        return packed.at[pl.ds(pl.multiple_of(owner * BLOCK, BLOCK), BLOCK)]

    def send_state(step, carry):
        owner = ((f // 16 + step // 16) % 2) * 16 + (f + step) % 16
        remote(own_state(owner), moved.at[f], s_send, s_recv, (owner, t)).start()
        return carry

    lax.fori_loop(1, 32, send_state, 0)
    moved[f] = packed[pl.ds(pl.multiple_of(f * BLOCK, BLOCK), BLOCK), :]
    for k in range(5):
        load_c[k].wait()

    def spread():
        pltpu.make_async_copy(moved.at[pl.ds(0, 31)], moved.at[pl.ds(0, 31)], s_recv).wait()
        lane = lax.broadcasted_iota(jnp.int32, (BLOCK, 128), 1)

        def half(h, carry):
            for group in range(5):
                value = [jnp.zeros((BLOCK, 128), jnp.float32)] * 3
                for g in range(16):
                    left = 40 * g - 128 * group
                    if left <= -40 or left >= 128:
                        continue
                    piece = moved[h * 16 + g].astype(jnp.float32)
                    here = (lane >= left) & (lane < left + 40)
                    for i in range(3):
                        shift = (left - 40 * i) % 128
                        rolled = pltpu.roll(piece, shift, 1) if shift else piece
                        value[i] = jnp.where(here, rolled, value[i])
                for i in range(3):
                    fresh[i, :, pl.ds(pl.multiple_of(h * 640 + group * 128, 128), 128)] = value[i]
            return carry

        lax.fori_loop(0, 2, half, 0)

    def base(color, stage):
        total = 0
        for s in range(stage):
            total = total + bits[ORDER[color][s]] * (8 >> s)
        return total

    def halving(wave, color, stage):
        half = 8 >> stage
        dim = ORDER[color][stage]
        return remote(
            part.at[wave, color, pl.ds(base(color, stage) + (1 - bits[dim]) * half, half)],
            recv.at[wave, color, pl.ds(SLOT[stage], half)],
            rs_send,
            rs_recv.at[wave, stage, color],
            cube_peer(dim),
        )

    def add(wave, color, stage, which):
        half = 8 >> stage
        bit = bits[ORDER[color][stage]]
        shift = (1 - bit if which else bit) * half
        own = pl.ds(base(color, stage) + shift, half)
        came = pl.ds(SLOT[stage - 1] + shift, half)
        part[wave, color, own] = (
            part[wave, color, own].astype(jnp.float32) + recv[wave, color, came].astype(jnp.float32)
        ).astype(BF)

    def x_target(wave):
        column = jnp.where(wave < 5, lo, 1 - lo)
        return at_device(lo, z, y, column, core)

    def x_copy(wave):
        k = wave % 5
        return remote(summed.at[wave], final.at[hi, k], x_send.at[wave], x_recv.at[hi, k], x_target(wave))

    stays = hi == lo
    my_rows = pl.multiple_of(f * BLOCK, BLOCK)

    def update(k, carry):
        for source in range(2):
            @pl.when(jnp.logical_not(stays & (hi == source)))
            def _(source=source):
                pltpu.make_async_copy(final.at[source, k], final.at[source, k], x_recv.at[source, k]).wait()

        for color in range(4):
            rows = pl.ds((color // 2) * 80, 80)
            columns = pl.ds(pl.multiple_of(k * WIDE + (color % 2) * 128, 128), 128)
            gradient = final[0, k, color].astype(jnp.float32) + final[1, k, color].astype(jnp.float32)
            new = adam_update(*(fresh[i, rows, columns] for i in range(3)), gradient)
            for i in range(3):
                fresh[i, rows, columns] = new[i]
            full[pl.ds(my_rows + (color // 2) * 80, 80), columns] = new[0].astype(BF)
        return carry

    def block(late, color, number):
        z_, y_ = z, y
        order = ORDER[color][::-1]
        for i in range(4):
            if number >> i & 1:
                dim = order[i]
                if dim < 2:
                    y_ = flip(y_, dim)
                else:
                    z_ = flip(z_, dim)
        owner = ((1 - lo if late else lo) * 4 + z_) * 4 + y_
        rows = pl.ds(pl.multiple_of(owner * BLOCK + (color // 2) * 80, 16), 80)
        return full.at[rows, pl.ds((color % 2) * 640, 640)]

    def forward(late, color, number, i):
        here = block(late, color, number)
        return remote(
            here, here, ag_send, ag_recv.at[late, color, number + (1 << i)], cube_peer(ORDER[color][::-1][i])
        )

    def arrived(late, color, number):
        here = block(late, color, number)
        pltpu.make_async_copy(here, here, ag_recv.at[late, color, number]).wait()

    def to_hi(late, color):
        here = block(late, color, 0)
        return remote(here, here, gx_send.at[color], ag_recv.at[late, color, 0], hi_peer)

    def roots(late, source):
        for color in range(4):
            if source:
                to_hi(late, color).start()
            else:
                arrived(late, color, 0)
            for i in (3, 2, 1, 0):
                forward(late, color, 0, i).start()

    def relay(late, number):
        for color in range(4):
            arrived(late, color, number)
            for i in (3, 2, 1):
                if number < 1 << i:
                    forward(late, color, number, i).start()

    def wave_at(now):
        return (now >= 0) & (now < WAVES), now

    def tick(now, carry):
        valid_4, wave_4 = wave_at(now - 5)

        @pl.when(valid_4)
        def _():
            for color in range(4):
                halving(wave_4, color, 3).wait_recv()
                summed[wave_4, color] = (
                    part[wave_4, color, base(color, 4)].astype(jnp.float32)
                    + recv[wave_4, color, SLOT[3]].astype(jnp.float32)
                ).astype(BF)

            @pl.when(stays & (wave_4 < 5))
            def _():
                final[hi, wave_4 % 5] = summed[wave_4]

            @pl.when(jnp.logical_not(stays & (wave_4 < 5)))
            def _():
                x_copy(wave_4).start()

        for stage in (3, 2, 1):
            valid, wave = wave_at(now - 1 - stage)

            @pl.when(valid)
            def _(wave=wave, stage=stage):
                for color in range(4):
                    halving(wave, color, stage - 1).wait_recv()
                    add(wave, color, stage, 1)
                    halving(wave, color, stage).start()
                    add(wave, color, stage, 0)

        valid_0, wave_0 = wave_at(now)

        @pl.when(valid_0)
        def _():
            for k in range(5):
                @pl.when(wave_0 == 5 + k)
                def _(k=k):
                    send_c[k].wait_recv()

            def rows(step, carry):
                @pl.when((now == 0) & (step == 2))
                def _():
                    send_a.wait_recv()
                    turn(near_row + 1024, 1 - core)

                quarter = (core * 2 + step) % 4
                left = at[pl.ds(pl.multiple_of(quarter * 640, 128), 640), :]
                product = jnp.dot(left, cot[wave_0], preferred_element_type=jnp.float32).astype(BF)
                for i in range(4):
                    for color in range(4):
                        top, side = i * BLOCK + (color // 2) * 80, (color % 2) * 128
                        part[wave_0, color, place(color, quarter, i)] = product[top : top + 80, side : side + 128]
                return carry

            lax.fori_loop(0, 4, rows, 0)
            for color in range(4):
                halving(wave_0, color, 0).start()

        for k, when in ((2, 1), (3, 3), (4, 4)):
            @pl.when(now == when)
            def _(k=k):
                send_c[k].start()

        @pl.when(now == 11)
        def _():
            spread()

        @pl.when(stays & (now == 12))
        def _():
            lax.fori_loop(0, 5, update, 0)
            roots(0, True)

        @pl.when(jnp.logical_not(stays) & (now == 13))
        def _():
            roots(0, False)

        @pl.when(now == jnp.where(stays, 13, 14))
        def _():
            relay(0, 1)

        return carry

    lax.fori_loop(0, WAVES + 5, tick, 0)

    @pl.when(jnp.logical_not(stays))
    def _():
        lax.fori_loop(0, 5, update, 0)
        roots(1, True)

    for number in range(2, 8):
        relay(0, number)

    @pl.when(stays)
    def _():
        roots(1, False)

    stores = [
        pltpu.make_async_copy(fresh.at[i], out, out_sem.at[i]) for i, out in enumerate((wn_out, mn_out, vn_out))
    ]
    for store in stores:
        store.start()
    for number in range(1, 4):
        relay(1, number)
    for number in range(8, 16):
        relay(0, number)
    early_rows = pl.ds(pl.multiple_of(lo * 2560, 128), 2560)
    late_rows = pl.ds(pl.multiple_of((1 - lo) * 2560, 128), 2560)
    store_early = pltpu.make_async_copy(full.at[early_rows], full_out.at[early_rows], out_sem.at[3])
    store_early.start()
    for number in range(4, 16):
        relay(1, number)
    store_late = pltpu.make_async_copy(full.at[late_rows], full_out.at[late_rows], out_sem.at[4])
    store_late.start()

    send_a.wait_send()
    pltpu.make_async_copy(packed.at[pl.ds(0, 4960)], packed.at[pl.ds(0, 4960)], s_send).wait()
    for k in range(5):
        send_c[k].wait_send()
    pltpu.make_async_copy(recv, recv, rs_send).wait()
    for wave in range(WAVES):
        if wave < 5:
            @pl.when(jnp.logical_not(stays))
            def _(wave=wave):
                x_copy(wave).wait_send()
        else:
            x_copy(wave).wait_send()
    for color in range(4):
        to_hi(0, color).wait_send()
    pltpu.make_async_copy(full.at[pl.ds(0, 4800)], full.at[pl.ds(0, 4800)], ag_send).wait()
    for store in stores:
        store.wait()
    store_early.wait()
    store_late.wait()


def copy_kernel(*refs):
    sources, targets, (small, large, in_sem, out_sem) = refs[:4], refs[4:8], refs[8:]
    pieces = [(sources[i], small.at[i], targets[i]) for i in range(3)]
    for i in range(10):
        rows = pl.ds(512 * i, 512)
        pieces.append((sources[3].at[rows], large.at[rows], targets[3].at[rows]))
    reads = [pltpu.make_async_copy(a, b, in_sem.at[i]) for i, (a, b, c) in enumerate(pieces)]
    writes = [pltpu.make_async_copy(b, c, out_sem.at[i]) for i, (a, b, c) in enumerate(pieces)]
    for read in reads:
        read.start()
    for read, write in zip(reads, writes):
        read.wait()
        write.start()
    for write in writes:
        write.wait()


def body(activations, cotangent, weights, first_moment, second_moment):
    any_space = pl.BlockSpec(memory_space=pl.ANY)
    shard = jax.ShapeDtypeStruct((BLOCK, 1280), jnp.float32)
    dma = pltpu.SemaphoreType.DMA
    results = pl.pallas_call(
        kernel,
        name="step",
        out_shape=(shard, shard, shard, jax.ShapeDtypeStruct((D, 1280), BF)),
        in_specs=[any_space] * 5,
        out_specs=(any_space,) * 4,
        scratch_shapes=[
            pltpu.VMEM((2560, 1024), BF),
            pltpu.VMEM((10, 1024, WIDE), BF),
            pltpu.VMEM((WAVES, 4, 16, 80, 128), BF),
            pltpu.VMEM((WAVES, 4, 15, 80, 128), BF),
            pltpu.VMEM((WAVES, 4, 80, 128), BF),
            pltpu.VMEM((2, 5, 4, 80, 128), BF),
            pltpu.VMEM((D, 1280), BF),
            pltpu.VMEM((3, BLOCK, 1280), jnp.float32),
            pltpu.VMEM((128, D), jnp.float32),
            pltpu.VMEM((D, 128), BF),
            pltpu.VMEM((32, BLOCK, 128), BF),
            dma((9,)), dma, dma, dma, dma, dma((5,)), dma((5,)), dma, dma((WAVES, 4, 4)), dma((WAVES,)), dma((2, 5)),
            dma, dma((2, 4, 16)), dma((4,)), dma((5,)),
        ],
        compiler_params=pltpu.CompilerParams(
            collective_id=0, has_side_effects=True, vmem_limit_bytes=67043328
        ),
        cost_estimate=pl.CostEstimate(flops=13_421_772_800, bytes_accessed=40_000_000, transcendentals=0),
    )(activations, cotangent, weights.T, first_moment.T, second_moment.T)
    return pl.pallas_call(
        copy_kernel,
        name="place",
        out_shape=(shard, shard, shard, jax.ShapeDtypeStruct((D, 1280), BF)),
        in_specs=[any_space] * 4,
        out_specs=(any_space,) * 4,
        scratch_shapes=[
            pltpu.VMEM((3, BLOCK, 1280), jnp.float32), pltpu.VMEM((D, 1280), BF), dma((13,)), dma((13,)),
        ],
    )(*results)


def solution(mesh):
    return jax.shard_map(
        body,
        mesh=mesh,
        in_specs=(
            P("fsdp", "tensor"),
            P("fsdp", "tensor"),
            P(None, ("tensor", "fsdp")),
            P(None, ("tensor", "fsdp")),
            P(None, ("tensor", "fsdp")),
        ),
        out_specs=(
            P("fsdp", "tensor"),
            P("fsdp", "tensor"),
            P("fsdp", "tensor"),
            P(None, "tensor"),
        ),
        check_vma=False,
    )
```

```python
import jax
import jax.numpy as jnp
from jax import lax
from jax.experimental import pallas as pl
from jax.experimental.pallas import tpu as pltpu
from jax.sharding import PartitionSpec as P

STEP = 20
D = 5120
BLOCK = 160
WAVES = 10
WIDE = 256
MESH = pl.DeviceIdType.MESH
BF = jnp.bfloat16

beta_one = 0.9
beta_two = 0.95
adam_eps = 1e-08
learn_rate = 0.0003
decay_rate = 0.1

ORDER = ((0, 2, 1, 3), (1, 3, 0, 2), (2, 1, 3, 0), (3, 0, 2, 1))
SLOT = (0, 8, 12, 14)


def adam_update(weights, first_moment, second_moment, gradient):
    first_new = beta_one * first_moment + (1.0 - beta_one) * gradient
    second_new = beta_two * second_moment + (1.0 - beta_two) * gradient * gradient
    corrected = first_new / (1.0 - beta_one**STEP)
    scaled = jnp.sqrt(second_new / (1.0 - beta_two**STEP)) + adam_eps
    weights_new = weights - learn_rate * (corrected / scaled + decay_rate * weights)
    return (weights_new, first_new, second_new)


def flip(value, dim):
    return value + 1 - 2 * (value % 2) if dim % 2 == 0 else 3 - value


def cube_bits(z, y):
    return ((y + y // 2) % 2, y // 2, (z + z // 2) % 2, z // 2)


def place(color, z, y):
    bits = cube_bits(z, y)
    order = ORDER[color]
    return bits[order[0]] * 8 + bits[order[1]] * 4 + bits[order[2]] * 2 + bits[order[3]]


def kernel(
    a_ref, c_ref, w_ref, m_ref, v_ref, fresh, full,
    at, cot, part, recv, summed, final, tall, packed, moved,
    load_sem, s_send, s_recv, a_send, a_recv, c_send, c_recv, rs_send, rs_recv, x_send, x_recv, ag_send, ag_recv,
    gx_send,
):
    f, t = lax.axis_index("fsdp"), lax.axis_index("tensor")
    hi, z, y = f // 16, (f // 4) % 4, f % 4
    lo, core = t // 2, t % 2

    def at_device(hi_, z_, y_, lo_, core_):
        return ((hi_ * 4 + z_) * 4 + y_, lo_ * 2 + core_)

    def cube_peer(dim):
        if dim < 2:
            return at_device(hi, z, flip(y, dim), lo, core)
        return at_device(hi, flip(z, dim), y, lo, core)

    def remote(src, dst, send, receive, device):
        return pltpu.make_async_remote_copy(
            src_ref=src, dst_ref=dst, send_sem=send, recv_sem=receive, device_id=device, device_id_type=MESH
        )

    bits = cube_bits(z, y)
    core_peer = at_device(hi, z, y, lo, 1 - core)
    lo_peer = at_device(hi, z, y, 1 - lo, core)
    hi_peer = at_device(1 - hi, z, y, lo, core)
    across = at_device(1 - hi, z, y, 1 - lo, core)

    barrier = pltpu.get_barrier_semaphore()
    for device in (core_peer, lo_peer, across):
        pl.semaphore_signal(barrier, inc=1, device_id=device, device_id_type=MESH)

    def greet(step, carry):
        pl.semaphore_signal(barrier, inc=1, device_id=((f + step) % 32, t), device_id_type=MESH)
        return carry

    lax.fori_loop(1, 32, greet, 0)

    near_row = pl.multiple_of(hi * 2560, 128)
    raw = [full.at[pl.ds(near_row, 1024)], full.at[pl.ds(near_row + 1024, 1024)]]
    send_a = remote(a_ref, raw[1], a_send, a_recv, core_peer)
    load_a = pltpu.make_async_copy(a_ref, raw[0], load_sem.at[0])
    load_a.start()
    load_s = [
        pltpu.make_async_copy(ref, tall.at[pl.ds(40 * i, 40)], load_sem.at[6 + i])
        for i, ref in enumerate((w_ref, m_ref, v_ref))
    ]
    for load in load_s:
        load.start()
    load_c = [
        pltpu.make_async_copy(c_ref.at[:, pl.ds(WIDE * k, WIDE)], cot.at[k], load_sem.at[1 + k]) for k in range(5)
    ]
    for k in range(5):
        load_c[k].start()
    send_c = [
        remote(c_ref.at[:, pl.ds(WIDE * k, WIDE)], cot.at[5 + k], c_send.at[k], c_recv.at[k], lo_peer)
        for k in range(5)
    ]
    def turn(start, core_):
        def step(i, carry):
            columns = pl.ds(pl.multiple_of(i * 128, 128), 128)
            rows = pl.ds(pl.multiple_of(core_ * 1280 + i * 128, 128), 128)
            at[rows, :] = full[pl.ds(start, 1024), columns].T
            return carry

        lax.fori_loop(0, 10, step, 0)

    load_a.wait()
    turn(near_row, core)

    tall[pl.ds(120, 8), :] = jnp.zeros((8, D), jnp.float32)
    for load in load_s:
        load.wait()

    def pack(i, carry):
        packed[pl.ds(pl.multiple_of(i * 512, 512), 512), :] = tall[:, pl.ds(pl.multiple_of(i * 512, 512), 512)].T.astype(BF)
        return carry

    lax.fori_loop(0, 10, pack, 0)

    pl.semaphore_wait(barrier, 34)
    send_a.start()
    send_c[0].start()
    send_c[1].start()

    def own_state(owner):
        return packed.at[pl.ds(pl.multiple_of(owner * BLOCK, BLOCK), BLOCK)]

    def send_state(step, carry):
        owner = ((f // 16 + step // 16) % 2) * 16 + (f + step) % 16
        remote(own_state(owner), moved.at[f], s_send, s_recv, (owner, t)).start()
        return carry

    lax.fori_loop(1, 32, send_state, 0)
    moved[f] = packed[pl.ds(pl.multiple_of(f * BLOCK, BLOCK), BLOCK), :]
    for k in range(5):
        load_c[k].wait()

    def spread():
        pltpu.make_async_copy(moved.at[pl.ds(0, 31)], moved.at[pl.ds(0, 31)], s_recv).wait()
        lane = lax.broadcasted_iota(jnp.int32, (BLOCK, 128), 1)

        def half(h, carry):
            for group in range(5):
                value = [jnp.zeros((BLOCK, 128), jnp.float32)] * 3
                for g in range(16):
                    left = 40 * g - 128 * group
                    if left <= -40 or left >= 128:
                        continue
                    piece = moved[h * 16 + g].astype(jnp.float32)
                    here = (lane >= left) & (lane < left + 40)
                    for i in range(3):
                        shift = (left - 40 * i) % 128
                        rolled = pltpu.roll(piece, shift, 1) if shift else piece
                        value[i] = jnp.where(here, rolled, value[i])
                for i in range(3):
                    fresh[i, :, pl.ds(pl.multiple_of(h * 640 + group * 128, 128), 128)] = value[i]
            return carry

        lax.fori_loop(0, 2, half, 0)

    def base(color, stage):
        total = 0
        for s in range(stage):
            total = total + bits[ORDER[color][s]] * (8 >> s)
        return total

    def halving(wave, color, stage):
        half = 8 >> stage
        dim = ORDER[color][stage]
        return remote(
            part.at[wave, color, pl.ds(base(color, stage) + (1 - bits[dim]) * half, half)],
            recv.at[wave, color, pl.ds(SLOT[stage], half)],
            rs_send,
            rs_recv.at[wave, stage, color],
            cube_peer(dim),
        )

    def add(wave, color, stage, which):
        half = 8 >> stage
        bit = bits[ORDER[color][stage]]
        shift = (1 - bit if which else bit) * half
        own = pl.ds(base(color, stage) + shift, half)
        came = pl.ds(SLOT[stage - 1] + shift, half)
        part[wave, color, own] = (
            part[wave, color, own].astype(jnp.float32) + recv[wave, color, came].astype(jnp.float32)
        ).astype(BF)

    def x_target(wave):
        column = jnp.where(wave < 5, lo, 1 - lo)
        return at_device(lo, z, y, column, core)

    def x_copy(wave):
        k = wave % 5
        return remote(summed.at[wave], final.at[hi, k], x_send.at[wave], x_recv.at[hi, k], x_target(wave))

    stays = hi == lo
    my_rows = pl.multiple_of(f * BLOCK, BLOCK)

    def update(k, carry):
        for source in range(2):
            @pl.when(jnp.logical_not(stays & (hi == source)))
            def _(source=source):
                pltpu.make_async_copy(final.at[source, k], final.at[source, k], x_recv.at[source, k]).wait()

        for color in range(4):
            rows = pl.ds((color // 2) * 80, 80)
            columns = pl.ds(pl.multiple_of(k * WIDE + (color % 2) * 128, 128), 128)
            gradient = final[0, k, color].astype(jnp.float32) + final[1, k, color].astype(jnp.float32)
            new = adam_update(*(fresh[i, rows, columns] for i in range(3)), gradient)
            for i in range(3):
                fresh[i, rows, columns] = new[i]
            full[pl.ds(my_rows + (color // 2) * 80, 80), columns] = new[0].astype(BF)
        return carry

    def block(late, color, number):
        z_, y_ = z, y
        order = ORDER[color][::-1]
        for i in range(4):
            if number >> i & 1:
                dim = order[i]
                if dim < 2:
                    y_ = flip(y_, dim)
                else:
                    z_ = flip(z_, dim)
        owner = ((1 - lo if late else lo) * 4 + z_) * 4 + y_
        rows = pl.ds(pl.multiple_of(owner * BLOCK + (color // 2) * 80, 16), 80)
        return full.at[rows, pl.ds((color % 2) * 640, 640)]

    def forward(late, color, number, i):
        here = block(late, color, number)
        return remote(
            here, here, ag_send, ag_recv.at[late, color, number + (1 << i)], cube_peer(ORDER[color][::-1][i])
        )

    def arrived(late, color, number):
        here = block(late, color, number)
        pltpu.make_async_copy(here, here, ag_recv.at[late, color, number]).wait()

    def to_hi(late, color):
        here = block(late, color, 0)
        return remote(here, here, gx_send.at[color], ag_recv.at[late, color, 0], hi_peer)

    def roots(late, source):
        for color in range(4):
            if source:
                to_hi(late, color).start()
            else:
                arrived(late, color, 0)
            for i in (3, 2, 1, 0):
                forward(late, color, 0, i).start()

    def relay(late, number):
        for color in range(4):
            arrived(late, color, number)
            for i in (3, 2, 1):
                if number < 1 << i:
                    forward(late, color, number, i).start()

    def wave_at(now):
        return (now >= 0) & (now < WAVES), now

    def tick(now, carry):
        valid_4, wave_4 = wave_at(now - 5)

        @pl.when(valid_4)
        def _():
            for color in range(4):
                halving(wave_4, color, 3).wait_recv()
                summed[wave_4, color] = (
                    part[wave_4, color, base(color, 4)].astype(jnp.float32)
                    + recv[wave_4, color, SLOT[3]].astype(jnp.float32)
                ).astype(BF)

            @pl.when(stays & (wave_4 < 5))
            def _():
                final[hi, wave_4 % 5] = summed[wave_4]

            @pl.when(jnp.logical_not(stays & (wave_4 < 5)))
            def _():
                x_copy(wave_4).start()

        for stage in (3, 2, 1):
            valid, wave = wave_at(now - 1 - stage)

            @pl.when(valid)
            def _(wave=wave, stage=stage):
                for color in range(4):
                    halving(wave, color, stage - 1).wait_recv()
                    add(wave, color, stage, 1)
                    halving(wave, color, stage).start()
                    add(wave, color, stage, 0)

        valid_0, wave_0 = wave_at(now)

        @pl.when(valid_0)
        def _():
            for k in range(5):
                @pl.when(wave_0 == 5 + k)
                def _(k=k):
                    send_c[k].wait_recv()

            def rows(step, carry):
                @pl.when((now == 0) & (step == 2))
                def _():
                    send_a.wait_recv()
                    turn(near_row + 1024, 1 - core)

                quarter = (core * 2 + step) % 4
                left = at[pl.ds(pl.multiple_of(quarter * 640, 128), 640), :]
                product = jnp.dot(left, cot[wave_0], preferred_element_type=jnp.float32).astype(BF)
                for i in range(4):
                    for color in range(4):
                        top, side = i * BLOCK + (color // 2) * 80, (color % 2) * 128
                        part[wave_0, color, place(color, quarter, i)] = product[top : top + 80, side : side + 128]
                return carry

            lax.fori_loop(0, 4, rows, 0)
            for color in range(4):
                halving(wave_0, color, 0).start()

        for k, when in ((2, 1), (3, 3), (4, 4)):
            @pl.when(now == when)
            def _(k=k):
                send_c[k].start()

        @pl.when(now == 11)
        def _():
            spread()

        @pl.when(stays & (now == 12))
        def _():
            lax.fori_loop(0, 5, update, 0)
            roots(0, True)

        @pl.when(jnp.logical_not(stays) & (now == 13))
        def _():
            roots(0, False)

        @pl.when(now == jnp.where(stays, 13, 14))
        def _():
            relay(0, 1)

        return carry

    lax.fori_loop(0, WAVES + 5, tick, 0)

    @pl.when(jnp.logical_not(stays))
    def _():
        lax.fori_loop(0, 5, update, 0)
        roots(1, True)

    for number in range(2, 8):
        relay(0, number)

    @pl.when(stays)
    def _():
        roots(1, False)

    for number in range(1, 4):
        relay(1, number)
    for number in range(8, 16):
        relay(0, number)
    for number in range(4, 16):
        relay(1, number)
    send_a.wait_send()
    pltpu.make_async_copy(packed.at[pl.ds(0, 4960)], packed.at[pl.ds(0, 4960)], s_send).wait()
    for k in range(5):
        send_c[k].wait_send()
    pltpu.make_async_copy(recv, recv, rs_send).wait()
    for wave in range(WAVES):
        if wave < 5:
            @pl.when(jnp.logical_not(stays))
            def _(wave=wave):
                x_copy(wave).wait_send()
        else:
            x_copy(wave).wait_send()
    for color in range(4):
        to_hi(0, color).wait_send()
    pltpu.make_async_copy(full.at[pl.ds(0, 4800)], full.at[pl.ds(0, 4800)], ag_send).wait()


def copy_kernel(fresh, full, wn_out, mn_out, vn_out, full_out, sem):
    copies = [pltpu.make_async_copy(fresh.at[i], out, sem.at[i]) for i, out in enumerate((wn_out, mn_out, vn_out))]
    for i in range(5):
        rows = pl.ds(1024 * i, 1024)
        copies.append(pltpu.make_async_copy(full.at[rows], full_out.at[rows], sem.at[3 + i]))
    for copy in copies:
        copy.start()
    for copy in copies:
        copy.wait()


def body(activations, cotangent, weights, first_moment, second_moment):
    any_space = pl.BlockSpec(memory_space=pl.ANY)
    shard = jax.ShapeDtypeStruct((BLOCK, 1280), jnp.float32)
    dma = pltpu.SemaphoreType.DMA
    results = pl.pallas_call(
        kernel,
        name="step",
        out_shape=(pltpu.VMEM((3, BLOCK, 1280), jnp.float32), pltpu.VMEM((D, 1280), BF)),
        in_specs=[any_space] * 5,
        out_specs=(pl.BlockSpec(memory_space=pltpu.VMEM),) * 2,
        scratch_shapes=[
            pltpu.VMEM((2560, 1024), BF),
            pltpu.VMEM((10, 1024, WIDE), BF),
            pltpu.VMEM((WAVES, 4, 16, 80, 128), BF),
            pltpu.VMEM((WAVES, 4, 15, 80, 128), BF),
            pltpu.VMEM((WAVES, 4, 80, 128), BF),
            pltpu.VMEM((2, 5, 4, 80, 128), BF),
            pltpu.VMEM((128, D), jnp.float32),
            pltpu.VMEM((D, 128), BF),
            pltpu.VMEM((32, BLOCK, 128), BF),
            dma((9,)), dma, dma, dma, dma, dma((5,)), dma((5,)), dma, dma((WAVES, 4, 4)), dma((WAVES,)), dma((2, 5)),
            dma, dma((2, 4, 16)), dma((4,)),
        ],
        compiler_params=pltpu.CompilerParams(
            collective_id=0, has_side_effects=True, vmem_limit_bytes=46 << 20
        ),
        cost_estimate=pl.CostEstimate(flops=13_421_772_800, bytes_accessed=40_000_000, transcendentals=0),
    )(activations, cotangent, weights.T, first_moment.T, second_moment.T)
    return pl.pallas_call(
        copy_kernel,
        name="place",
        out_shape=(shard, shard, shard, jax.ShapeDtypeStruct((D, 1280), BF)),
        in_specs=[pl.BlockSpec(memory_space=pltpu.VMEM)] * 2,
        out_specs=(any_space,) * 4,
        scratch_shapes=[dma((8,))],
        compiler_params=pltpu.CompilerParams(vmem_limit_bytes=1 << 20),
    )(*results)


def solution(mesh):
    return jax.shard_map(
        body,
        mesh=mesh,
        in_specs=(
            P("fsdp", "tensor"),
            P("fsdp", "tensor"),
            P(None, ("tensor", "fsdp")),
            P(None, ("tensor", "fsdp")),
            P(None, ("tensor", "fsdp")),
        ),
        out_specs=(
            P("fsdp", "tensor"),
            P("fsdp", "tensor"),
            P("fsdp", "tensor"),
            P(None, "tensor"),
        ),
        check_vma=False,
    )
```

```python
import jax
import jax.numpy as jnp
from jax import lax
from jax.experimental import pallas as pl
from jax.experimental.pallas import tpu as pltpu
from jax.sharding import PartitionSpec as P

STEP = 20
D = 5120
BLOCK = 160
WAVES = 10
WIDE = 256
SIDE = (256, 128)
MESH = pl.DeviceIdType.MESH
BF = jnp.bfloat16

beta_one = 0.9
beta_two = 0.95
adam_eps = 1e-08
learn_rate = 0.0003
decay_rate = 0.1

ORDER = ((0, 2, 1, 3), (1, 3, 0, 2), (2, 1, 3, 0), (3, 0, 2, 1))
SLOT = (0, 8, 12, 14)


def adam_update(weights, first_moment, second_moment, gradient):
    first_new = beta_one * first_moment + (1.0 - beta_one) * gradient
    second_new = beta_two * second_moment + (1.0 - beta_two) * gradient * gradient
    corrected = first_new / (1.0 - beta_one**STEP)
    scaled = jnp.sqrt(second_new / (1.0 - beta_two**STEP)) + adam_eps
    weights_new = weights - learn_rate * (corrected / scaled + decay_rate * weights)
    return (weights_new, first_new, second_new)


def flip(value, dim):
    return value + 1 - 2 * (value % 2) if dim % 2 == 0 else 3 - value


def cube_bits(z, y):
    return ((y + y // 2) % 2, y // 2, (z + z // 2) % 2, z // 2)


def place(color, z, y):
    bits = cube_bits(z, y)
    order = ORDER[color]
    return bits[order[0]] * 8 + bits[order[1]] * 4 + bits[order[2]] * 2 + bits[order[3]]


def kernel(
    a_ref, c_ref, w_ref, m_ref, v_ref, fresh, full,
    at, cot, part, recv, summed, final, tall, packed, moved,
    load_sem, s_send, s_recv, a_send, a_recv, c_send, c_recv, rs_send, rs_recv, x_send, x_recv, ag_send, ag_recv,
    gx_send, side_send, side_recv,
):
    f, t = lax.axis_index("fsdp"), lax.axis_index("tensor")
    hi, z, y = f // 16, (f // 4) % 4, f % 4
    lo, core = t // 2, t % 2

    def at_device(hi_, z_, y_, lo_, core_):
        return ((hi_ * 4 + z_) * 4 + y_, lo_ * 2 + core_)

    def cube_peer(dim):
        if dim < 2:
            return at_device(hi, z, flip(y, dim), lo, core)
        return at_device(hi, flip(z, dim), y, lo, core)

    def remote(src, dst, send, receive, device):
        return pltpu.make_async_remote_copy(
            src_ref=src, dst_ref=dst, send_sem=send, recv_sem=receive, device_id=device, device_id_type=MESH
        )

    bits = cube_bits(z, y)
    core_peer = at_device(hi, z, y, lo, 1 - core)
    lo_peer = at_device(hi, z, y, 1 - lo, core)
    hi_peer = at_device(1 - hi, z, y, lo, core)
    across = at_device(1 - hi, z, y, 1 - lo, core)

    barrier = pltpu.get_barrier_semaphore()
    for device in (core_peer, lo_peer, across):
        pl.semaphore_signal(barrier, inc=1, device_id=device, device_id_type=MESH)

    def greet(step, carry):
        pl.semaphore_signal(barrier, inc=1, device_id=((f + step) % 32, t), device_id_type=MESH)
        return carry

    lax.fori_loop(1, 32, greet, 0)

    near_row = pl.multiple_of(hi * 2560, 128)
    raw = [full.at[pl.ds(near_row, 1024)], full.at[pl.ds(near_row + 1024, 1024)]]
    send_a = remote(a_ref, raw[1], a_send, a_recv, core_peer)
    load_a = pltpu.make_async_copy(a_ref, raw[0], load_sem.at[0])
    load_a.start()
    load_s = [
        pltpu.make_async_copy(ref, tall.at[pl.ds(40 * i, 40)], load_sem.at[6 + i])
        for i, ref in enumerate((w_ref, m_ref, v_ref))
    ]
    for load in load_s:
        load.start()
    load_c = [
        pltpu.make_async_copy(c_ref.at[:, pl.ds(WIDE * k, WIDE)], cot.at[k], load_sem.at[1 + k]) for k in range(5)
    ]
    for k in range(5):
        load_c[k].start()
    send_c = [
        remote(c_ref.at[:, pl.ds(WIDE * k, WIDE)], cot.at[5 + k], c_send.at[k], c_recv.at[k], lo_peer)
        for k in range(5)
    ]
    def turn(start, core_):
        def step(i, carry):
            columns = pl.ds(pl.multiple_of(i * 128, 128), 128)
            rows = pl.ds(pl.multiple_of(core_ * 1280 + i * 128, 128), 128)
            at[rows, :] = full[pl.ds(start, 1024), columns].T
            return carry

        lax.fori_loop(0, 10, step, 0)

    load_a.wait()
    turn(near_row, core)

    tall[pl.ds(120, 8), :] = jnp.zeros((8, D), jnp.float32)
    for load in load_s:
        load.wait()

    def pack(i, carry):
        packed[pl.ds(pl.multiple_of(i * 512, 512), 512), :] = tall[:, pl.ds(pl.multiple_of(i * 512, 512), 512)].T.astype(BF)
        return carry

    lax.fori_loop(0, 10, pack, 0)

    pl.semaphore_wait(barrier, 34)
    send_a.start()
    for k in range(5):
        send_c[k].start()

    def own_state(owner):
        return packed.at[pl.ds(pl.multiple_of(owner * BLOCK, BLOCK), BLOCK)]

    def send_state(step, carry):
        owner = ((f // 16 + step // 16) % 2) * 16 + (f + step) % 16
        remote(own_state(owner), moved.at[f], s_send, s_recv, (owner, t)).start()
        return carry

    lax.fori_loop(1, 16, send_state, 0)
    moved[f] = packed[pl.ds(pl.multiple_of(f * BLOCK, BLOCK), BLOCK), :]
    for k in range(5):
        load_c[k].wait()

    def spread():
        pltpu.make_async_copy(moved.at[pl.ds(0, 31)], moved.at[pl.ds(0, 31)], s_recv).wait()
        lane = lax.broadcasted_iota(jnp.int32, (BLOCK, 128), 1)

        def half(h, carry):
            for group in range(5):
                value = [jnp.zeros((BLOCK, 128), jnp.float32)] * 3
                for g in range(16):
                    left = 40 * g - 128 * group
                    if left <= -40 or left >= 128:
                        continue
                    piece = moved[h * 16 + g].astype(jnp.float32)
                    here = (lane >= left) & (lane < left + 40)
                    for i in range(3):
                        shift = (left - 40 * i) % 128
                        rolled = pltpu.roll(piece, shift, 1) if shift else piece
                        value[i] = jnp.where(here, rolled, value[i])
                for i in range(3):
                    fresh[i, :, pl.ds(pl.multiple_of(h * 640 + group * 128, 128), 128)] = value[i]
            return carry

        lax.fori_loop(0, 2, half, 0)

    def base(color, stage):
        total = 0
        for s in range(stage):
            total = total + bits[ORDER[color][s]] * (8 >> s)
        return total

    def halving(wave, color, stage):
        half = 8 >> stage
        dim = ORDER[color][stage]
        return remote(
            part.at[wave, color, pl.ds(base(color, stage) + (1 - bits[dim]) * half, half)],
            recv.at[wave, color, pl.ds(SLOT[stage], half)],
            rs_send,
            rs_recv.at[wave, stage, color],
            cube_peer(dim),
        )

    def add(wave, color, stage, which):
        half = 8 >> stage
        bit = bits[ORDER[color][stage]]
        shift = (1 - bit if which else bit) * half
        own = pl.ds(base(color, stage) + shift, half)
        came = pl.ds(SLOT[stage - 1] + shift, half)
        part[wave, color, own] = (
            part[wave, color, own].astype(jnp.float32) + recv[wave, color, came].astype(jnp.float32)
        ).astype(BF)

    def x_target(wave):
        column = jnp.where(wave < 5, lo, 1 - lo)
        return at_device(lo, z, y, column, core)

    def x_copy(wave):
        k = wave % 5
        return remote(summed.at[wave], final.at[hi, k], x_send.at[wave], x_recv.at[hi, k], x_target(wave))

    stays = hi == lo
    my_rows = pl.multiple_of(f * BLOCK, BLOCK)

    def update(k, carry):
        for source in range(2):
            @pl.when(jnp.logical_not(stays & (hi == source)))
            def _(source=source):
                pltpu.make_async_copy(final.at[source, k], final.at[source, k], x_recv.at[source, k]).wait()

        for color in range(4):
            rows = pl.ds((color // 2) * 80, 80)
            columns = pl.ds(pl.multiple_of(k * WIDE + (color % 2) * 128, 128), 128)
            gradient = final[0, k, color].astype(jnp.float32) + final[1, k, color].astype(jnp.float32)
            new = adam_update(*(fresh[i, rows, columns] for i in range(3)), gradient)
            for i in range(3):
                fresh[i, rows, columns] = new[i]
            full[pl.ds(my_rows + (color // 2) * 80, 80), columns] = new[0].astype(BF)
        return carry

    def block(late, color, number, piece):
        z_, y_ = z, y
        order = ORDER[color][::-1]
        for i in range(4):
            if number >> i & 1:
                dim = order[i]
                if dim < 2:
                    y_ = flip(y_, dim)
                else:
                    z_ = flip(z_, dim)
        owner = ((1 - lo if late else lo) * 4 + z_) * 4 + y_
        rows = pl.ds(pl.multiple_of(owner * BLOCK + (color // 2) * 80, 16), 80)
        start = (color % 2) * 640
        columns = {
            "all": (start, 640), "main": (start, 640 - SIDE[late]), "side": (start + 640 - SIDE[late], SIDE[late])
        }[piece]
        return full.at[rows, pl.ds(*columns)]

    def landing(late, color, number, piece):
        return rs_recv.at[number // 4, number % 4, color] if piece == "side" else ag_recv.at[late, color, number]

    def forward(late, color, number, i, piece):
        here = block(late, color, number, piece)
        there = landing(late, color, number + (1 << i), piece)
        return remote(here, here, ag_send, there, cube_peer(ORDER[color][::-1][i]))

    def arrived(late, color, number, piece):
        here = block(late, color, number, piece)
        pltpu.make_async_copy(here, here, landing(late, color, number, piece)).wait()

    def to_hi(late, color):
        here = block(late, color, 0, "main")
        return remote(here, here, gx_send.at[color], ag_recv.at[late, color, 0], hi_peer)

    def side(late, color, number):
        here = block(late, color, number, "side")
        return remote(here, here, side_send, side_recv, hi_peer)

    def roots(late, color, piece):
        for i in (3, 2, 1, 0):
            forward(late, color, 0, i, piece).start()

    def relay(late, number, piece, across):
        for color in range(4):
            arrived(late, color, number, piece)
            for i in (3, 2, 1):
                if number < 1 << i:
                    forward(late, color, number, i, piece).start()
            if across:
                side(late, color, number).start()

    def early_roots():
        for color in range(4):
            to_hi(0, color).start()
            roots(0, color, "all")
        for color in range(4):
            side(0, color, 0).start()

    def late_roots():
        for color in range(4):
            to_hi(1, color).start()
        for color in range(4):
            roots(1, color, "side")
            side(1, color, 0).start()
        for color in range(4):
            roots(1, color, "main")

    def other_roots(late):
        for color in range(4):
            arrived(late, color, 0, "main")
            roots(late, color, "main")

    def wave_at(now):
        return (now >= 0) & (now < WAVES), now

    def tick(now, carry):
        valid_4, wave_4 = wave_at(now - 5)

        @pl.when(valid_4)
        def _():
            for color in range(4):
                halving(wave_4, color, 3).wait_recv()
                summed[wave_4, color] = (
                    part[wave_4, color, base(color, 4)].astype(jnp.float32)
                    + recv[wave_4, color, SLOT[3]].astype(jnp.float32)
                ).astype(BF)

            @pl.when(stays & (wave_4 < 5))
            def _():
                final[hi, wave_4 % 5] = summed[wave_4]

            @pl.when(jnp.logical_not(stays & (wave_4 < 5)))
            def _():
                x_copy(wave_4).start()

        for stage in (3, 2, 1):
            valid, wave = wave_at(now - 1 - stage)

            @pl.when(valid)
            def _(wave=wave, stage=stage):
                for color in range(4):
                    halving(wave, color, stage - 1).wait_recv()
                    add(wave, color, stage, 1)
                    halving(wave, color, stage).start()
                    add(wave, color, stage, 0)

        valid_0, wave_0 = wave_at(now)

        @pl.when(valid_0)
        def _():
            for k in range(5):
                @pl.when(wave_0 == 5 + k)
                def _(k=k):
                    send_c[k].wait_recv()

            def rows(step, carry):
                @pl.when((now == 0) & (step == 2))
                def _():
                    send_a.wait_recv()
                    turn(near_row + 1024, 1 - core)

                quarter = (core * 2 + step) % 4
                left = at[pl.ds(pl.multiple_of(quarter * 640, 128), 640), :]
                product = jnp.dot(left, cot[wave_0], preferred_element_type=jnp.float32).astype(BF)
                for i in range(4):
                    for color in range(4):
                        top, side = i * BLOCK + (color // 2) * 80, (color % 2) * 128
                        part[wave_0, color, place(color, quarter, i)] = product[top : top + 80, side : side + 128]
                return carry

            lax.fori_loop(0, 4, rows, 0)
            for color in range(4):
                halving(wave_0, color, 0).start()

        @pl.when(now == 4)
        def _():
            lax.fori_loop(16, 32, send_state, 0)

        @pl.when(now == 11)
        def _():
            spread()

        @pl.when(stays & (now == 12))
        def _():
            lax.fori_loop(0, 5, update, 0)
            early_roots()

        @pl.when(jnp.logical_not(stays) & (now == 13))
        def _():
            other_roots(0)

        @pl.when(stays & (now == 13))
        def _():
            relay(0, 1, "all", True)

        @pl.when(jnp.logical_not(stays) & (now == 14))
        def _():
            relay(0, 1, "main", False)

        return carry

    lax.fori_loop(0, WAVES + 5, tick, 0)

    def arrived_across(late):
        rows = full.at[pl.ds(0, SIDE[late] * 4)]
        pltpu.make_async_copy(rows, rows, side_recv).wait()

    @pl.when(stays)
    def _():
        for number in range(2, 8):
            relay(0, number, "all", True)
        other_roots(1)
        for number in range(8, 16):
            relay(0, number, "all", True)
        for number in range(1, 16):
            relay(1, number, "main", False)
        arrived_across(1)

    @pl.when(jnp.logical_not(stays))
    def _():
        lax.fori_loop(0, 5, update, 0)
        late_roots()
        for number in range(2, 4):
            relay(0, number, "main", False)
        for number in range(1, 4):
            relay(1, number, "side", True)
        for number in range(4, 8):
            relay(0, number, "main", False)
        for number in range(4, 16):
            relay(1, number, "side", True)
        for number in range(1, 4):
            relay(1, number, "main", False)
        for number in range(8, 16):
            relay(0, number, "main", False)
        for number in range(4, 16):
            relay(1, number, "main", False)
        arrived_across(0)

    send_a.wait_send()
    pltpu.make_async_copy(packed.at[pl.ds(0, 4960)], packed.at[pl.ds(0, 4960)], s_send).wait()
    for k in range(5):
        send_c[k].wait_send()
    pltpu.make_async_copy(recv, recv, rs_send).wait()
    for wave in range(WAVES):
        if wave < 5:
            @pl.when(jnp.logical_not(stays))
            def _(wave=wave):
                x_copy(wave).wait_send()
        else:
            x_copy(wave).wait_send()
    for late in range(2):
        @pl.when(stays if late == 0 else jnp.logical_not(stays))
        def _(late=late):
            for color in range(4):
                to_hi(late, color).wait_send()
            side_rows = full.at[pl.ds(0, SIDE[late] * 4)]
            pltpu.make_async_copy(side_rows, side_rows, side_send).wait()
            tree_rows = full.at[pl.ds(0, 60 * 80 * (1280 - SIDE[1 - late]) // 1280)]
            pltpu.make_async_copy(tree_rows, tree_rows, ag_send).wait()


def copy_kernel(fresh, full, wn_out, mn_out, vn_out, full_out, sem):
    copies = [pltpu.make_async_copy(fresh.at[i], out, sem.at[i]) for i, out in enumerate((wn_out, mn_out, vn_out))]
    for i in range(5):
        rows = pl.ds(1024 * i, 1024)
        copies.append(pltpu.make_async_copy(full.at[rows], full_out.at[rows], sem.at[3 + i]))
    for copy in copies:
        copy.start()
    for copy in copies:
        copy.wait()


def body(activations, cotangent, weights, first_moment, second_moment):
    any_space = pl.BlockSpec(memory_space=pl.ANY)
    shard = jax.ShapeDtypeStruct((BLOCK, 1280), jnp.float32)
    dma = pltpu.SemaphoreType.DMA
    results = pl.pallas_call(
        kernel,
        name="step",
        out_shape=(pltpu.VMEM((3, BLOCK, 1280), jnp.float32), pltpu.VMEM((D, 1280), BF)),
        in_specs=[any_space] * 5,
        out_specs=(pl.BlockSpec(memory_space=pltpu.VMEM),) * 2,
        scratch_shapes=[
            pltpu.VMEM((2560, 1024), BF),
            pltpu.VMEM((10, 1024, WIDE), BF),
            pltpu.VMEM((WAVES, 4, 16, 80, 128), BF),
            pltpu.VMEM((WAVES, 4, 15, 80, 128), BF),
            pltpu.VMEM((WAVES, 4, 80, 128), BF),
            pltpu.VMEM((2, 5, 4, 80, 128), BF),
            pltpu.VMEM((128, D), jnp.float32),
            pltpu.VMEM((D, 128), BF),
            pltpu.VMEM((32, BLOCK, 128), BF),
            dma((9,)), dma, dma, dma, dma, dma((5,)), dma((5,)), dma, dma((WAVES, 4, 4)), dma((WAVES,)), dma((2, 5)),
            dma, dma((2, 4, 16)), dma((4,)), dma, dma,
        ],
        compiler_params=pltpu.CompilerParams(
            collective_id=0, has_side_effects=True, vmem_limit_bytes=46 << 20
        ),
        cost_estimate=pl.CostEstimate(flops=13_421_772_800, bytes_accessed=40_000_000, transcendentals=0),
    )(activations, cotangent, weights.T, first_moment.T, second_moment.T)
    return pl.pallas_call(
        copy_kernel,
        name="place",
        out_shape=(shard, shard, shard, jax.ShapeDtypeStruct((D, 1280), BF)),
        in_specs=[pl.BlockSpec(memory_space=pltpu.VMEM)] * 2,
        out_specs=(any_space,) * 4,
        scratch_shapes=[dma((8,))],
        compiler_params=pltpu.CompilerParams(vmem_limit_bytes=1 << 20),
    )(*results)


def solution(mesh):
    return jax.shard_map(
        body,
        mesh=mesh,
        in_specs=(
            P("fsdp", "tensor"),
            P("fsdp", "tensor"),
            P(None, ("tensor", "fsdp")),
            P(None, ("tensor", "fsdp")),
            P(None, ("tensor", "fsdp")),
        ),
        out_specs=(
            P("fsdp", "tensor"),
            P("fsdp", "tensor"),
            P("fsdp", "tensor"),
            P(None, "tensor"),
        ),
        check_vma=False,
    )
```

```python
import jax
import jax.numpy as jnp
from jax import lax
from jax.experimental import pallas as pl
from jax.experimental.pallas import tpu as pltpu
from jax.sharding import PartitionSpec as P

STEP = 20
D = 5120
BLOCK = 160
WAVES = 10
WIDE = 256
SIDE = ((256, 256, 128, 128), (256, 256, 128, 128))
MESH = pl.DeviceIdType.MESH
BF = jnp.bfloat16

beta_one = 0.9
beta_two = 0.95
adam_eps = 1e-08
learn_rate = 0.0003
decay_rate = 0.1

ORDER = ((0, 2, 1, 3), (1, 3, 0, 2), (2, 1, 3, 0), (3, 0, 2, 1))
SLOT = (0, 8, 12, 14)


def adam_update(weights, first_moment, second_moment, gradient):
    first_new = beta_one * first_moment + (1.0 - beta_one) * gradient
    second_new = beta_two * second_moment + (1.0 - beta_two) * gradient * gradient
    corrected = first_new / (1.0 - beta_one**STEP)
    scaled = jnp.sqrt(second_new / (1.0 - beta_two**STEP)) + adam_eps
    weights_new = weights - learn_rate * (corrected / scaled + decay_rate * weights)
    return (weights_new, first_new, second_new)


def flip(value, dim):
    return value + 1 - 2 * (value % 2) if dim % 2 == 0 else 3 - value


def cube_bits(z, y):
    return ((y + y // 2) % 2, y // 2, (z + z // 2) % 2, z // 2)


def place(color, z, y):
    bits = cube_bits(z, y)
    order = ORDER[color]
    return bits[order[0]] * 8 + bits[order[1]] * 4 + bits[order[2]] * 2 + bits[order[3]]


def kernel(
    a_ref, c_ref, w_ref, m_ref, v_ref, fresh, full,
    at, cot, part, recv, summed, final, tall, packed, moved,
    load_sem, s_send, s_recv, a_send, a_recv, c_send, c_recv, rs_send, rs_recv, x_send, x_recv, ag_send, ag_recv,
    gx_send, side_send, side_recv,
):
    f, t = lax.axis_index("fsdp"), lax.axis_index("tensor")
    hi, z, y = f // 16, (f // 4) % 4, f % 4
    lo, core = t // 2, t % 2

    def at_device(hi_, z_, y_, lo_, core_):
        return ((hi_ * 4 + z_) * 4 + y_, lo_ * 2 + core_)

    def cube_peer(dim):
        if dim < 2:
            return at_device(hi, z, flip(y, dim), lo, core)
        return at_device(hi, flip(z, dim), y, lo, core)

    def remote(src, dst, send, receive, device):
        return pltpu.make_async_remote_copy(
            src_ref=src, dst_ref=dst, send_sem=send, recv_sem=receive, device_id=device, device_id_type=MESH
        )

    bits = cube_bits(z, y)
    core_peer = at_device(hi, z, y, lo, 1 - core)
    lo_peer = at_device(hi, z, y, 1 - lo, core)
    hi_peer = at_device(1 - hi, z, y, lo, core)
    across = at_device(1 - hi, z, y, 1 - lo, core)

    barrier = pltpu.get_barrier_semaphore()
    for device in (core_peer, lo_peer, across):
        pl.semaphore_signal(barrier, inc=1, device_id=device, device_id_type=MESH)

    def greet(step, carry):
        pl.semaphore_signal(barrier, inc=1, device_id=((f + step) % 32, t), device_id_type=MESH)
        return carry

    lax.fori_loop(1, 32, greet, 0)

    near_row = pl.multiple_of(hi * 2560, 128)
    raw = [full.at[pl.ds(near_row, 1024)], full.at[pl.ds(near_row + 1024, 1024)]]
    send_a = remote(a_ref, raw[1], a_send, a_recv, core_peer)
    load_a = pltpu.make_async_copy(a_ref, raw[0], load_sem.at[0])
    load_a.start()
    load_s = [
        pltpu.make_async_copy(ref, tall.at[pl.ds(40 * i, 40)], load_sem.at[6 + i])
        for i, ref in enumerate((w_ref, m_ref, v_ref))
    ]
    for load in load_s:
        load.start()
    load_c = [
        pltpu.make_async_copy(c_ref.at[:, pl.ds(WIDE * k, WIDE)], cot.at[k], load_sem.at[1 + k]) for k in range(5)
    ]
    for k in range(5):
        load_c[k].start()
    send_c = [
        remote(c_ref.at[:, pl.ds(WIDE * k, WIDE)], cot.at[5 + k], c_send.at[k], c_recv.at[k], lo_peer)
        for k in range(5)
    ]
    def turn(start, core_):
        def step(i, carry):
            columns = pl.ds(pl.multiple_of(i * 128, 128), 128)
            rows = pl.ds(pl.multiple_of(core_ * 1280 + i * 128, 128), 128)
            at[rows, :] = full[pl.ds(start, 1024), columns].T
            return carry

        lax.fori_loop(0, 10, step, 0)

    load_a.wait()
    turn(near_row, core)

    tall[pl.ds(120, 8), :] = jnp.zeros((8, D), jnp.float32)
    for load in load_s:
        load.wait()

    def pack(i, carry):
        packed[pl.ds(pl.multiple_of(i * 512, 512), 512), :] = tall[:, pl.ds(pl.multiple_of(i * 512, 512), 512)].T.astype(BF)
        return carry

    lax.fori_loop(0, 10, pack, 0)

    pl.semaphore_wait(barrier, 34)
    send_a.start()
    for k in range(5):
        send_c[k].start()

    def own_state(owner):
        return packed.at[pl.ds(pl.multiple_of(owner * BLOCK, BLOCK), BLOCK)]

    def send_state(step, carry):
        owner = ((f // 16 + step // 16) % 2) * 16 + (f + step) % 16
        remote(own_state(owner), moved.at[f], s_send, s_recv, (owner, t)).start()
        return carry

    lax.fori_loop(1, 16, send_state, 0)
    moved[f] = packed[pl.ds(pl.multiple_of(f * BLOCK, BLOCK), BLOCK), :]
    for k in range(5):
        load_c[k].wait()

    def spread():
        pltpu.make_async_copy(moved.at[pl.ds(0, 31)], moved.at[pl.ds(0, 31)], s_recv).wait()
        lane = lax.broadcasted_iota(jnp.int32, (BLOCK, 128), 1)

        def half(h, carry):
            for group in range(5):
                value = [jnp.zeros((BLOCK, 128), jnp.float32)] * 3
                for g in range(16):
                    left = 40 * g - 128 * group
                    if left <= -40 or left >= 128:
                        continue
                    piece = moved[h * 16 + g].astype(jnp.float32)
                    here = (lane >= left) & (lane < left + 40)
                    for i in range(3):
                        shift = (left - 40 * i) % 128
                        rolled = pltpu.roll(piece, shift, 1) if shift else piece
                        value[i] = jnp.where(here, rolled, value[i])
                for i in range(3):
                    fresh[i, :, pl.ds(pl.multiple_of(h * 640 + group * 128, 128), 128)] = value[i]
            return carry

        lax.fori_loop(0, 2, half, 0)

    def base(color, stage):
        total = 0
        for s in range(stage):
            total = total + bits[ORDER[color][s]] * (8 >> s)
        return total

    def halving(wave, color, stage):
        half = 8 >> stage
        dim = ORDER[color][stage]
        return remote(
            part.at[wave, color, pl.ds(base(color, stage) + (1 - bits[dim]) * half, half)],
            recv.at[wave, color, pl.ds(SLOT[stage], half)],
            rs_send,
            rs_recv.at[wave, stage, color],
            cube_peer(dim),
        )

    def add(wave, color, stage, which):
        half = 8 >> stage
        bit = bits[ORDER[color][stage]]
        shift = (1 - bit if which else bit) * half
        own = pl.ds(base(color, stage) + shift, half)
        came = pl.ds(SLOT[stage - 1] + shift, half)
        part[wave, color, own] = (
            part[wave, color, own].astype(jnp.float32) + recv[wave, color, came].astype(jnp.float32)
        ).astype(BF)

    def x_target(wave):
        column = jnp.where(wave < 5, lo, 1 - lo)
        return at_device(lo, z, y, column, core)

    def x_copy(wave):
        k = wave % 5
        return remote(summed.at[wave], final.at[hi, k], x_send.at[wave], x_recv.at[hi, k], x_target(wave))

    stays = hi == lo
    my_rows = pl.multiple_of(f * BLOCK, BLOCK)

    def update(k, carry):
        for source in range(2):
            @pl.when(jnp.logical_not(stays & (hi == source)))
            def _(source=source):
                pltpu.make_async_copy(final.at[source, k], final.at[source, k], x_recv.at[source, k]).wait()

        for color in range(4):
            rows = pl.ds((color // 2) * 80, 80)
            columns = pl.ds(pl.multiple_of(k * WIDE + (color % 2) * 128, 128), 128)
            gradient = final[0, k, color].astype(jnp.float32) + final[1, k, color].astype(jnp.float32)
            new = adam_update(*(fresh[i, rows, columns] for i in range(3)), gradient)
            for i in range(3):
                fresh[i, rows, columns] = new[i]
            full[pl.ds(my_rows + (color // 2) * 80, 80), columns] = new[0].astype(BF)
        return carry

    def block(late, color, number, piece):
        z_, y_ = z, y
        order = ORDER[color][::-1]
        for i in range(4):
            if number >> i & 1:
                dim = order[i]
                if dim < 2:
                    y_ = flip(y_, dim)
                else:
                    z_ = flip(z_, dim)
        owner = ((1 - lo if late else lo) * 4 + z_) * 4 + y_
        rows = pl.ds(pl.multiple_of(owner * BLOCK + (color // 2) * 80, 16), 80)
        start, width = (color % 2) * 640, SIDE[late][color]
        columns = {
            "all": (start, 640), "main": (start, 640 - width), "side": (start + 640 - width, width)
        }[piece]
        return full.at[rows, pl.ds(*columns)]

    def landing(late, color, number, piece):
        return rs_recv.at[number // 4, number % 4, color] if piece == "side" else ag_recv.at[late, color, number]

    def forward(late, color, number, i, piece):
        here = block(late, color, number, piece)
        there = landing(late, color, number + (1 << i), piece)
        return remote(here, here, ag_send, there, cube_peer(ORDER[color][::-1][i]))

    def arrived(late, color, number, piece):
        here = block(late, color, number, piece)
        pltpu.make_async_copy(here, here, landing(late, color, number, piece)).wait()

    def to_hi(late, color):
        here = block(late, color, 0, "main")
        return remote(here, here, gx_send.at[color], ag_recv.at[late, color, 0], hi_peer)

    def side(late, color, number):
        here = block(late, color, number, "side")
        return remote(here, here, side_send, side_recv, hi_peer)

    def roots(late, color, piece):
        for i in (3, 2, 1, 0):
            forward(late, color, 0, i, piece).start()

    def relay(late, number, piece, across):
        for color in range(4):
            arrived(late, color, number, piece)
            for i in (3, 2, 1):
                if number < 1 << i:
                    forward(late, color, number, i, piece).start()
            if across:
                side(late, color, number).start()

    def late_roots():
        for color in range(4):
            to_hi(1, color).start()
        for color in range(4):
            roots(1, color, "side")
            side(1, color, 0).start()

    def other_roots(late):
        for color in range(4):
            arrived(late, color, 0, "main")
            roots(late, color, "main")

    def wave_at(now):
        return (now >= 0) & (now < WAVES), now

    def tick(now, carry):
        valid_4, wave_4 = wave_at(now - 5)

        @pl.when(valid_4)
        def _():
            for color in range(4):
                halving(wave_4, color, 3).wait_recv()
                summed[wave_4, color] = (
                    part[wave_4, color, base(color, 4)].astype(jnp.float32)
                    + recv[wave_4, color, SLOT[3]].astype(jnp.float32)
                ).astype(BF)

            @pl.when(stays & (wave_4 < 5))
            def _():
                final[hi, wave_4 % 5] = summed[wave_4]

            @pl.when(jnp.logical_not(stays & (wave_4 < 5)))
            def _():
                x_copy(wave_4).start()

        for stage in (3, 2, 1):
            valid, wave = wave_at(now - 1 - stage)

            @pl.when(valid)
            def _(wave=wave, stage=stage):
                for color in range(4):
                    halving(wave, color, stage - 1).wait_recv()
                    add(wave, color, stage, 1)
                    halving(wave, color, stage).start()
                    add(wave, color, stage, 0)

        valid_0, wave_0 = wave_at(now)

        @pl.when(valid_0)
        def _():
            for k in range(5):
                @pl.when(wave_0 == 5 + k)
                def _(k=k):
                    send_c[k].wait_recv()

            def rows(step, carry):
                @pl.when((now == 0) & (step == 2))
                def _():
                    send_a.wait_recv()
                    turn(near_row + 1024, 1 - core)

                quarter = (core * 2 + step) % 4
                left = at[pl.ds(pl.multiple_of(quarter * 640, 128), 640), :]
                product = jnp.dot(left, cot[wave_0], preferred_element_type=jnp.float32).astype(BF)
                for i in range(4):
                    for color in range(4):
                        top, side = i * BLOCK + (color // 2) * 80, (color % 2) * 128
                        part[wave_0, color, place(color, quarter, i)] = product[top : top + 80, side : side + 128]
                return carry

            lax.fori_loop(0, 4, rows, 0)
            for color in range(4):
                halving(wave_0, color, 0).start()

        @pl.when(now == 4)
        def _():
            lax.fori_loop(16, 32, send_state, 0)

        @pl.when(now == 10)
        def _():
            spread()

        @pl.when(stays & (now == 11))
        def _():
            lax.fori_loop(0, 5, update, 0)
            for color in range(4):
                to_hi(0, color).start()
            for color in range(4):
                side(0, color, 0).start()
            roots(0, 0, "all")

        @pl.when(jnp.logical_not(stays) & (now == 13))
        def _():
            other_roots(0)

        @pl.when(stays & (now == 12))
        def _():
            roots(0, 1, "all")

        @pl.when(stays & (now == 13))
        def _():
            for color in range(2, 4):
                roots(0, color, "all")

        @pl.when(stays & (now == 14))
        def _():
            relay(0, 1, "all", True)

        @pl.when(jnp.logical_not(stays) & (now == 14))
        def _():
            relay(0, 1, "main", False)

        return carry

    lax.fori_loop(0, WAVES + 5, tick, 0)

    def arrived_across(late):
        rows = full.at[pl.ds(0, sum(SIDE[late]))]
        pltpu.make_async_copy(rows, rows, side_recv).wait()

    @pl.when(stays)
    def _():
        for number in range(2, 8):
            relay(0, number, "all", True)
        other_roots(1)
        for number in range(8, 16):
            relay(0, number, "all", True)
        for number in range(1, 16):
            relay(1, number, "main", False)
        arrived_across(1)

    @pl.when(jnp.logical_not(stays))
    def _():
        lax.fori_loop(0, 5, update, 0)
        late_roots()
        for number in range(2, 4):
            relay(0, number, "main", False)
        for number in range(1, 8):
            relay(1, number, "side", True)
        for color in range(4):
            roots(1, color, "main")
        for number in range(4, 8):
            relay(0, number, "main", False)
        for number in range(8, 16):
            relay(1, number, "side", True)
        for number in range(1, 4):
            relay(1, number, "main", False)
        for number in range(8, 16):
            relay(0, number, "main", False)
        for number in range(4, 16):
            relay(1, number, "main", False)
        arrived_across(0)

    send_a.wait_send()
    pltpu.make_async_copy(packed.at[pl.ds(0, 4960)], packed.at[pl.ds(0, 4960)], s_send).wait()
    for k in range(5):
        send_c[k].wait_send()
    pltpu.make_async_copy(recv, recv, rs_send).wait()
    for wave in range(WAVES):
        if wave < 5:
            @pl.when(jnp.logical_not(stays))
            def _(wave=wave):
                x_copy(wave).wait_send()
        else:
            x_copy(wave).wait_send()
    for late in range(2):
        @pl.when(stays if late == 0 else jnp.logical_not(stays))
        def _(late=late):
            for color in range(4):
                to_hi(late, color).wait_send()
            side_rows = full.at[pl.ds(0, sum(SIDE[late]))]
            pltpu.make_async_copy(side_rows, side_rows, side_send).wait()
            tree_rows = full.at[pl.ds(0, 15 * 80 * (5120 - sum(SIDE[1 - late])) // 1280)]
            pltpu.make_async_copy(tree_rows, tree_rows, ag_send).wait()


def copy_kernel(fresh, full, wn_out, mn_out, vn_out, full_out, sem):
    copies = [pltpu.make_async_copy(fresh.at[i], out, sem.at[i]) for i, out in enumerate((wn_out, mn_out, vn_out))]
    for i in range(5):
        rows = pl.ds(1024 * i, 1024)
        copies.append(pltpu.make_async_copy(full.at[rows], full_out.at[rows], sem.at[3 + i]))
    for copy in copies:
        copy.start()
    for copy in copies:
        copy.wait()


def body(activations, cotangent, weights, first_moment, second_moment):
    any_space = pl.BlockSpec(memory_space=pl.ANY)
    shard = jax.ShapeDtypeStruct((BLOCK, 1280), jnp.float32)
    dma = pltpu.SemaphoreType.DMA
    results = pl.pallas_call(
        kernel,
        name="step",
        out_shape=(pltpu.VMEM((3, BLOCK, 1280), jnp.float32), pltpu.VMEM((D, 1280), BF)),
        in_specs=[any_space] * 5,
        out_specs=(pl.BlockSpec(memory_space=pltpu.VMEM),) * 2,
        scratch_shapes=[
            pltpu.VMEM((2560, 1024), BF),
            pltpu.VMEM((10, 1024, WIDE), BF),
            pltpu.VMEM((WAVES, 4, 16, 80, 128), BF),
            pltpu.VMEM((WAVES, 4, 15, 80, 128), BF),
            pltpu.VMEM((WAVES, 4, 80, 128), BF),
            pltpu.VMEM((2, 5, 4, 80, 128), BF),
            pltpu.VMEM((128, D), jnp.float32),
            pltpu.VMEM((D, 128), BF),
            pltpu.VMEM((32, BLOCK, 128), BF),
            dma((9,)), dma, dma, dma, dma, dma((5,)), dma((5,)), dma, dma((WAVES, 4, 4)), dma((WAVES,)), dma((2, 5)),
            dma, dma((2, 4, 16)), dma((4,)), dma, dma,
        ],
        compiler_params=pltpu.CompilerParams(
            collective_id=0, has_side_effects=True, vmem_limit_bytes=46 << 20
        ),
        cost_estimate=pl.CostEstimate(flops=13_421_772_800, bytes_accessed=40_000_000, transcendentals=0),
    )(activations, cotangent, weights.T, first_moment.T, second_moment.T)
    return pl.pallas_call(
        copy_kernel,
        name="place",
        out_shape=(shard, shard, shard, jax.ShapeDtypeStruct((D, 1280), BF)),
        in_specs=[pl.BlockSpec(memory_space=pltpu.VMEM)] * 2,
        out_specs=(any_space,) * 4,
        scratch_shapes=[dma((8,))],
        compiler_params=pltpu.CompilerParams(vmem_limit_bytes=1 << 20),
    )(*results)


def solution(mesh):
    return jax.shard_map(
        body,
        mesh=mesh,
        in_specs=(
            P("fsdp", "tensor"),
            P("fsdp", "tensor"),
            P(None, ("tensor", "fsdp")),
            P(None, ("tensor", "fsdp")),
            P(None, ("tensor", "fsdp")),
        ),
        out_specs=(
            P("fsdp", "tensor"),
            P("fsdp", "tensor"),
            P("fsdp", "tensor"),
            P(None, "tensor"),
        ),
        check_vma=False,
    )
```

```python
import jax
import jax.numpy as jnp
from jax import lax
from jax.experimental import pallas as pl
from jax.experimental.pallas import tpu as pltpu
from jax.sharding import PartitionSpec as P

STEP = 20
D = 5120
BLOCK = 160
WAVES = 10
WIDE = 256
SIDE = ((256, 256, 128, 128), (256, 256, 128, 128))
MESH = pl.DeviceIdType.MESH
BF = jnp.bfloat16

beta_one = 0.9
beta_two = 0.95
adam_eps = 1e-08
learn_rate = 0.0003
decay_rate = 0.1

ORDER = ((0, 2, 1, 3), (1, 3, 0, 2), (2, 1, 3, 0), (3, 0, 2, 1))
SLOT = (0, 8, 12, 14)


def adam_update(weights, first_moment, second_moment, gradient):
    first_new = beta_one * first_moment + (1.0 - beta_one) * gradient
    second_new = beta_two * second_moment + (1.0 - beta_two) * gradient * gradient
    corrected = first_new / (1.0 - beta_one**STEP)
    scaled = jnp.sqrt(second_new / (1.0 - beta_two**STEP)) + adam_eps
    weights_new = weights - learn_rate * (corrected / scaled + decay_rate * weights)
    return (weights_new, first_new, second_new)


def flip(value, dim):
    return value + 1 - 2 * (value % 2) if dim % 2 == 0 else 3 - value


def cube_bits(z, y):
    return ((y + y // 2) % 2, y // 2, (z + z // 2) % 2, z // 2)


def place(color, z, y):
    bits = cube_bits(z, y)
    order = ORDER[color]
    return bits[order[0]] * 8 + bits[order[1]] * 4 + bits[order[2]] * 2 + bits[order[3]]


def kernel(
    a_ref, c_ref, w_ref, m_ref, v_ref, fresh, full,
    at, cot, part, recv, summed, final, tall, packed, moved,
    load_sem, s_send, s_recv, a_send, a_recv, c_send, c_recv, rs_send, rs_recv, x_send, x_recv, ag_send, ag_recv,
    gx_send, side_send, side_recv,
):
    f, t = lax.axis_index("fsdp"), lax.axis_index("tensor")
    hi, z, y = f // 16, (f // 4) % 4, f % 4
    lo, core = t // 2, t % 2

    def at_device(hi_, z_, y_, lo_, core_):
        return ((hi_ * 4 + z_) * 4 + y_, lo_ * 2 + core_)

    def cube_peer(dim):
        if dim < 2:
            return at_device(hi, z, flip(y, dim), lo, core)
        return at_device(hi, flip(z, dim), y, lo, core)

    def remote(src, dst, send, receive, device):
        return pltpu.make_async_remote_copy(
            src_ref=src, dst_ref=dst, send_sem=send, recv_sem=receive, device_id=device, device_id_type=MESH
        )

    bits = cube_bits(z, y)
    core_peer = at_device(hi, z, y, lo, 1 - core)
    lo_peer = at_device(hi, z, y, 1 - lo, core)
    hi_peer = at_device(1 - hi, z, y, lo, core)
    across = at_device(1 - hi, z, y, 1 - lo, core)

    barrier = pltpu.get_barrier_semaphore()
    for device in (core_peer, lo_peer, across):
        pl.semaphore_signal(barrier, inc=1, device_id=device, device_id_type=MESH)

    def greet(step, carry):
        pl.semaphore_signal(barrier, inc=1, device_id=((f + step) % 32, t), device_id_type=MESH)
        return carry

    lax.fori_loop(1, 32, greet, 0)

    near_row = pl.multiple_of(hi * 2560, 128)
    raw = [full.at[pl.ds(near_row, 1024)], full.at[pl.ds(near_row + 1024, 1024)]]
    send_a = remote(a_ref, raw[1], a_send, a_recv, core_peer)
    load_a = pltpu.make_async_copy(a_ref, raw[0], load_sem.at[0])
    load_a.start()
    load_s = [
        pltpu.make_async_copy(ref, tall.at[pl.ds(40 * i, 40)], load_sem.at[6 + i])
        for i, ref in enumerate((w_ref, m_ref, v_ref))
    ]
    for load in load_s:
        load.start()
    load_c = [
        pltpu.make_async_copy(c_ref.at[:, pl.ds(WIDE * k, WIDE)], cot.at[k], load_sem.at[1 + k]) for k in range(5)
    ]
    for k in range(5):
        load_c[k].start()
    send_c = [
        remote(c_ref.at[:, pl.ds(WIDE * k, WIDE)], cot.at[5 + k], c_send.at[k], c_recv.at[k], lo_peer)
        for k in range(5)
    ]
    def turn(start, core_):
        def step(i, carry):
            columns = pl.ds(pl.multiple_of(i * 128, 128), 128)
            rows = pl.ds(pl.multiple_of(core_ * 1280 + i * 128, 128), 128)
            at[rows, :] = full[pl.ds(start, 1024), columns].T
            return carry

        lax.fori_loop(0, 10, step, 0)

    load_a.wait()
    turn(near_row, core)

    tall[pl.ds(120, 8), :] = jnp.zeros((8, D), jnp.float32)
    for load in load_s:
        load.wait()

    def pack(i, carry):
        packed[pl.ds(pl.multiple_of(i * 512, 512), 512), :] = tall[:, pl.ds(pl.multiple_of(i * 512, 512), 512)].T.astype(BF)
        return carry

    lax.fori_loop(0, 10, pack, 0)

    pl.semaphore_wait(barrier, 34)
    send_a.start()
    for k in range(5):
        send_c[k].start()

    def own_state(owner):
        return packed.at[pl.ds(pl.multiple_of(owner * BLOCK, BLOCK), BLOCK)]

    def send_state(step, carry):
        owner = ((f // 16 + step // 16) % 2) * 16 + (f + step) % 16
        remote(own_state(owner), moved.at[f], s_send, s_recv, (owner, t)).start()
        return carry

    lax.fori_loop(1, 16, send_state, 0)
    moved[f] = packed[pl.ds(pl.multiple_of(f * BLOCK, BLOCK), BLOCK), :]
    for k in range(5):
        load_c[k].wait()

    def spread():
        pltpu.make_async_copy(moved.at[pl.ds(0, 31)], moved.at[pl.ds(0, 31)], s_recv).wait()
        lane = lax.broadcasted_iota(jnp.int32, (BLOCK, 128), 1)

        def half(h, carry):
            for group in range(5):
                value = [jnp.zeros((BLOCK, 128), jnp.float32)] * 3
                for g in range(16):
                    left = 40 * g - 128 * group
                    if left <= -40 or left >= 128:
                        continue
                    piece = moved[h * 16 + g].astype(jnp.float32)
                    here = (lane >= left) & (lane < left + 40)
                    for i in range(3):
                        shift = (left - 40 * i) % 128
                        rolled = pltpu.roll(piece, shift, 1) if shift else piece
                        value[i] = jnp.where(here, rolled, value[i])
                for i in range(3):
                    fresh[i, :, pl.ds(pl.multiple_of(h * 640 + group * 128, 128), 128)] = value[i]
            return carry

        lax.fori_loop(0, 2, half, 0)

    def base(color, stage):
        total = 0
        for s in range(stage):
            total = total + bits[ORDER[color][s]] * (8 >> s)
        return total

    def halving(wave, color, stage):
        half = 8 >> stage
        dim = ORDER[color][stage]
        return remote(
            part.at[wave, color, pl.ds(base(color, stage) + (1 - bits[dim]) * half, half)],
            recv.at[wave, color, pl.ds(SLOT[stage], half)],
            rs_send,
            rs_recv.at[wave, stage, color],
            cube_peer(dim),
        )

    def add(wave, color, stage, which):
        half = 8 >> stage
        bit = bits[ORDER[color][stage]]
        shift = (1 - bit if which else bit) * half
        own = pl.ds(base(color, stage) + shift, half)
        came = pl.ds(SLOT[stage - 1] + shift, half)
        part[wave, color, own] = (
            part[wave, color, own].astype(jnp.float32) + recv[wave, color, came].astype(jnp.float32)
        ).astype(BF)

    def x_target(wave):
        column = jnp.where(wave < 5, lo, 1 - lo)
        return at_device(lo, z, y, column, core)

    def x_copy(wave):
        k = wave % 5
        return remote(summed.at[wave], final.at[hi, k], x_send.at[wave], x_recv.at[hi, k], x_target(wave))

    stays = hi == lo
    my_rows = pl.multiple_of(f * BLOCK, BLOCK)

    def update(k, carry):
        for source in range(2):
            @pl.when(jnp.logical_not(stays & (hi == source)))
            def _(source=source):
                pltpu.make_async_copy(final.at[source, k], final.at[source, k], x_recv.at[source, k]).wait()

        for color in range(4):
            rows = pl.ds((color // 2) * 80, 80)
            columns = pl.ds(pl.multiple_of(k * WIDE + (color % 2) * 128, 128), 128)
            gradient = final[0, k, color].astype(jnp.float32) + final[1, k, color].astype(jnp.float32)
            new = adam_update(*(fresh[i, rows, columns] for i in range(3)), gradient)
            for i in range(3):
                fresh[i, rows, columns] = new[i]
            full[pl.ds(my_rows + (color // 2) * 80, 80), columns] = new[0].astype(BF)
        return carry

    def block(late, color, number, piece):
        z_, y_ = z, y
        order = ORDER[color][::-1]
        for i in range(4):
            if number >> i & 1:
                dim = order[i]
                if dim < 2:
                    y_ = flip(y_, dim)
                else:
                    z_ = flip(z_, dim)
        owner = ((1 - lo if late else lo) * 4 + z_) * 4 + y_
        rows = pl.ds(pl.multiple_of(owner * BLOCK + (color // 2) * 80, 16), 80)
        start, width = (color % 2) * 640, SIDE[late][color]
        columns = {
            "all": (start, 640), "main": (start, 640 - width), "side": (start + 640 - width, width)
        }[piece]
        return full.at[rows, pl.ds(*columns)]

    def landing(late, color, number, piece):
        if late and piece != "side":
            return ag_recv.at[color, number]
        return rs_recv.at[(4 if late else 0) + number // 4, number % 4, color]

    def forward(late, color, number, i, piece):
        here = block(late, color, number, piece)
        there = landing(late, color, number + (1 << i), piece)
        return remote(here, here, ag_send, there, cube_peer(ORDER[color][::-1][i]))

    def arrived(late, color, number, piece):
        here = block(late, color, number, piece)
        pltpu.make_async_copy(here, here, landing(late, color, number, piece)).wait()

    def to_hi(late, color):
        here = block(late, color, 0, "main")
        return remote(here, here, gx_send.at[color], landing(late, color, 0, "main"), hi_peer)

    def side(late, color, number):
        here = block(late, color, number, "side")
        return remote(here, here, side_send, side_recv, hi_peer)

    def roots(late, color, piece):
        for i in (3, 2, 1, 0):
            forward(late, color, 0, i, piece).start()

    def relay(late, number, piece, across):
        for color in range(4):
            arrived(late, color, number, piece)
            for i in (3, 2, 1):
                if number < 1 << i:
                    forward(late, color, number, i, piece).start()
            if across:
                side(late, color, number).start()

    def late_roots():
        for color in range(4):
            to_hi(1, color).start()
        for color in range(4):
            roots(1, color, "side")
            side(1, color, 0).start()

    def other_roots(late):
        for color in range(4):
            arrived(late, color, 0, "main")
            roots(late, color, "main")

    def wave_at(now):
        return (now >= 0) & (now < WAVES), now

    def tick(now, carry):
        valid_4, wave_4 = wave_at(now - 5)

        @pl.when(valid_4)
        def _():
            for color in range(4):
                halving(wave_4, color, 3).wait_recv()
                summed[wave_4, color] = (
                    part[wave_4, color, base(color, 4)].astype(jnp.float32)
                    + recv[wave_4, color, SLOT[3]].astype(jnp.float32)
                ).astype(BF)

            @pl.when(stays & (wave_4 < 5))
            def _():
                final[hi, wave_4 % 5] = summed[wave_4]

            @pl.when(jnp.logical_not(stays & (wave_4 < 5)))
            def _():
                x_copy(wave_4).start()

        for stage in (3, 2, 1):
            valid, wave = wave_at(now - 1 - stage)

            @pl.when(valid)
            def _(wave=wave, stage=stage):
                for color in range(4):
                    halving(wave, color, stage - 1).wait_recv()
                    add(wave, color, stage, 1)
                    halving(wave, color, stage).start()
                    add(wave, color, stage, 0)

        valid_0, wave_0 = wave_at(now)

        @pl.when(valid_0)
        def _():
            for k in range(5):
                @pl.when(wave_0 == 5 + k)
                def _(k=k):
                    send_c[k].wait_recv()

            def rows(step, carry):
                @pl.when((now == 0) & (step == 2))
                def _():
                    send_a.wait_recv()
                    turn(near_row + 1024, 1 - core)

                quarter = (core * 2 + step) % 4
                left = at[pl.ds(pl.multiple_of(quarter * 640, 128), 640), :]
                product = jnp.dot(left, cot[wave_0], preferred_element_type=jnp.float32).astype(BF)
                for i in range(4):
                    for color in range(4):
                        top, side = i * BLOCK + (color // 2) * 80, (color % 2) * 128
                        part[wave_0, color, place(color, quarter, i)] = product[top : top + 80, side : side + 128]
                return carry

            lax.fori_loop(0, 4, rows, 0)
            for color in range(4):
                halving(wave_0, color, 0).start()

        @pl.when(now == 4)
        def _():
            lax.fori_loop(16, 32, send_state, 0)

        @pl.when(now == 10)
        def _():
            spread()

        @pl.when(stays & (now == 11))
        def _():
            lax.fori_loop(0, 5, update, 0)
            for color in range(4):
                to_hi(0, color).start()
            for color in range(4):
                side(0, color, 0).start()
            roots(0, 0, "all")

        @pl.when(jnp.logical_not(stays) & (now == 13))
        def _():
            other_roots(0)

        @pl.when(stays & (now == 12))
        def _():
            roots(0, 1, "all")

        @pl.when(stays & (now == 13))
        def _():
            for color in range(2, 4):
                roots(0, color, "all")

        @pl.when(stays & (now == 14))
        def _():
            relay(0, 1, "all", True)

        @pl.when(jnp.logical_not(stays) & (now == 14))
        def _():
            relay(0, 1, "main", False)

        return carry

    lax.fori_loop(0, WAVES + 5, tick, 0)

    def arrived_across(late):
        rows = full.at[pl.ds(0, sum(SIDE[late]))]
        pltpu.make_async_copy(rows, rows, side_recv).wait()

    @pl.when(stays)
    def _():
        for number in range(2, 8):
            relay(0, number, "all", True)
        other_roots(1)
        for number in range(8, 16):
            relay(0, number, "all", True)
        for number in range(1, 16):
            relay(1, number, "main", False)
        arrived_across(1)

    @pl.when(jnp.logical_not(stays))
    def _():
        lax.fori_loop(0, 5, update, 0)
        late_roots()
        for number in range(2, 4):
            relay(0, number, "main", False)
        for number in range(1, 8):
            relay(1, number, "side", True)
        for color in range(4):
            roots(1, color, "main")
        for number in range(4, 8):
            relay(0, number, "main", False)
        for number in range(8, 16):
            relay(1, number, "side", True)
        for number in range(1, 4):
            relay(1, number, "main", False)
        for number in range(8, 16):
            relay(0, number, "main", False)
        for number in range(4, 16):
            relay(1, number, "main", False)
        arrived_across(0)

    send_a.wait_send()
    pltpu.make_async_copy(packed.at[pl.ds(0, 4960)], packed.at[pl.ds(0, 4960)], s_send).wait()
    for k in range(5):
        send_c[k].wait_send()
    pltpu.make_async_copy(recv, recv, rs_send).wait()
    for wave in range(WAVES):
        if wave < 5:
            @pl.when(jnp.logical_not(stays))
            def _(wave=wave):
                x_copy(wave).wait_send()
        else:
            x_copy(wave).wait_send()
    for late in range(2):
        @pl.when(stays if late == 0 else jnp.logical_not(stays))
        def _(late=late):
            for color in range(4):
                to_hi(late, color).wait_send()
            side_rows = full.at[pl.ds(0, sum(SIDE[late]))]
            pltpu.make_async_copy(side_rows, side_rows, side_send).wait()
            tree_rows = full.at[pl.ds(0, 15 * 80 * (5120 - sum(SIDE[1 - late])) // 1280)]
            pltpu.make_async_copy(tree_rows, tree_rows, ag_send).wait()


def copy_kernel(fresh, full, wn_out, mn_out, vn_out, full_out, sem):
    copies = [pltpu.make_async_copy(fresh.at[i], out, sem.at[i]) for i, out in enumerate((wn_out, mn_out, vn_out))]
    for i in range(5):
        rows = pl.ds(1024 * i, 1024)
        copies.append(pltpu.make_async_copy(full.at[rows], full_out.at[rows], sem.at[3 + i]))
    for copy in copies:
        copy.start()
    for copy in copies:
        copy.wait()


def body(activations, cotangent, weights, first_moment, second_moment):
    any_space = pl.BlockSpec(memory_space=pl.ANY)
    shard = jax.ShapeDtypeStruct((BLOCK, 1280), jnp.float32)
    dma = pltpu.SemaphoreType.DMA
    results = pl.pallas_call(
        kernel,
        name="step",
        out_shape=(pltpu.VMEM((3, BLOCK, 1280), jnp.float32), pltpu.VMEM((D, 1280), BF)),
        in_specs=[any_space] * 5,
        out_specs=(pl.BlockSpec(memory_space=pltpu.VMEM),) * 2,
        scratch_shapes=[
            pltpu.VMEM((2560, 1024), BF),
            pltpu.VMEM((10, 1024, WIDE), BF),
            pltpu.VMEM((WAVES, 4, 16, 80, 128), BF),
            pltpu.VMEM((WAVES, 4, 15, 80, 128), BF),
            pltpu.VMEM((WAVES, 4, 80, 128), BF),
            pltpu.VMEM((2, 5, 4, 80, 128), BF),
            pltpu.VMEM((128, D), jnp.float32),
            pltpu.VMEM((D, 128), BF),
            pltpu.VMEM((32, BLOCK, 128), BF),
            dma((9,)), dma, dma, dma, dma, dma((5,)), dma((5,)), dma, dma((WAVES, 4, 4)), dma((WAVES,)), dma((2, 5)),
            dma, dma((4, 16)), dma((4,)), dma, dma,
        ],
        compiler_params=pltpu.CompilerParams(
            collective_id=0, has_side_effects=True, vmem_limit_bytes=46 << 20
        ),
        cost_estimate=pl.CostEstimate(flops=13_421_772_800, bytes_accessed=40_000_000, transcendentals=0),
    )(activations, cotangent, weights.T, first_moment.T, second_moment.T)
    return pl.pallas_call(
        copy_kernel,
        name="place",
        out_shape=(shard, shard, shard, jax.ShapeDtypeStruct((D, 1280), BF)),
        in_specs=[pl.BlockSpec(memory_space=pltpu.VMEM)] * 2,
        out_specs=(any_space,) * 4,
        scratch_shapes=[dma((8,))],
        compiler_params=pltpu.CompilerParams(vmem_limit_bytes=1 << 20),
    )(*results)


def solution(mesh):
    return jax.shard_map(
        body,
        mesh=mesh,
        in_specs=(
            P("fsdp", "tensor"),
            P("fsdp", "tensor"),
            P(None, ("tensor", "fsdp")),
            P(None, ("tensor", "fsdp")),
            P(None, ("tensor", "fsdp")),
        ),
        out_specs=(
            P("fsdp", "tensor"),
            P("fsdp", "tensor"),
            P("fsdp", "tensor"),
            P(None, "tensor"),
        ),
        check_vma=False,
    )
```
